16 devices in a mesh: data: 16 (over z, y, x, core).
Axes of the slice: x: 2, y: 2, z: 2, core: 2. Of those that a mesh axis runs over, the one named last changes fastest.
Arguments:
- act_in: bfloat16 [65536, 896], P('data')
- grad_out: bfloat16 [65536, 896], P('data')
- w_up: bfloat16 [2, 896, 4864], replicated
- w_down: bfloat16 [2, 4864, 896], replicated
- master_up: float32 [2, 896, 4864], P(None, 'data')
- master_down: float32 [2, 4864, 896], P(None, 'data')
- exp_avg_up: float32 [2, 896, 4864], P(None, 'data')
- exp_avg_down: float32 [2, 4864, 896], P(None, 'data')
- exp_sq_up: float32 [2, 896, 4864], P(None, 'data')
- exp_sq_down: float32 [2, 4864, 896], P(None, 'data')
- learn_rate: float32 [], replicated
- clip_norm: float32 [], replicated
Outputs:
- output 1: bfloat16 [2, 896, 4864], replicated
- output 2: bfloat16 [2, 4864, 896], replicated
- output 3: float32 [2, 896, 4864], P(None, 'data')
- output 4: float32 [2, 4864, 896], P(None, 'data')
- output 5: float32 [2, 896, 4864], P(None, 'data')
- output 6: float32 [2, 4864, 896], P(None, 'data')
- output 7: float32 [2, 896, 4864], P(None, 'data')
- output 8: float32 [2, 4864, 896], P(None, 'data')
- output 9: float32 [], replicated
All inputs are finite; a program needn't handle non-finite values.
Results may differ from the reference program's by a relative error of at most 0.00407.
Values are sent between devices in bfloat16 or wider.
A program may use at most 1 GiB of HBM per device.

```python
import jax
import jax.numpy as jnp
from jax import lax

D = 896
FF = 4864
TOKENS_DEV = 4096
GROUP = 16
STEP = 10

BETA_ONE = 0.9
BETA_TWO = 0.95
ADAM_EPS = 1e-8
NORM_EPS = 1e-6
INV_SQRT_TWO = 0.7071067811865476
INV_SQRT_TWO_PI = 0.3989422804014327


def gelu_parts(pre_act):
    normal_cdf = 0.5 * (1.0 + lax.erf(pre_act * INV_SQRT_TWO))
    normal_pdf = jnp.exp(-0.5 * pre_act * pre_act) * INV_SQRT_TWO_PI
    return pre_act * normal_cdf, normal_cdf + pre_act * normal_pdf


def block_grads(act_blk, out_blk, w_up, w_down):
    z_one = jnp.dot(act_blk, w_up[0], preferred_element_type=jnp.float32)
    gelu_one, slope_one = gelu_parts(z_one)
    act_one = gelu_one.astype(jnp.bfloat16)
    hidden = jnp.dot(act_one, w_down[0], preferred_element_type=jnp.float32).astype(jnp.bfloat16)
    z_three = jnp.dot(hidden, w_up[1], preferred_element_type=jnp.float32)
    gelu_three, slope_three = gelu_parts(z_three)
    act_three = gelu_three.astype(jnp.bfloat16)
    g_four = jnp.dot(act_three.T, out_blk, preferred_element_type=jnp.float32)
    dz_three = (jnp.dot(out_blk, w_down[1].T, preferred_element_type=jnp.float32) * slope_three).astype(jnp.bfloat16)
    g_three = jnp.dot(hidden.T, dz_three, preferred_element_type=jnp.float32)
    d_hidden = jnp.dot(dz_three, w_up[1].T, preferred_element_type=jnp.float32).astype(jnp.bfloat16)
    g_two = jnp.dot(act_one.T, d_hidden, preferred_element_type=jnp.float32)
    dz_one = (jnp.dot(d_hidden, w_down[0].T, preferred_element_type=jnp.float32) * slope_one).astype(jnp.bfloat16)
    g_one = jnp.dot(act_blk.T, dz_one, preferred_element_type=jnp.float32)
    return jnp.stack([g_one, g_three]), jnp.stack([g_two, g_four])


def full_grads(act_in, grad_out, w_up, w_down):
    act_blocks = act_in.reshape(GROUP, TOKENS_DEV, D)
    out_blocks = grad_out.reshape(GROUP, TOKENS_DEV, D)

    def add_block(carry_sums, blocks):
        grad_up, grad_down = block_grads(blocks[0], blocks[1], w_up, w_down)
        return (carry_sums[0] + grad_up, carry_sums[1] + grad_down), None

    start_sums = (jnp.zeros((2, D, FF), jnp.float32), jnp.zeros((2, FF, D), jnp.float32))
    final_sums = lax.scan(add_block, start_sums, (act_blocks, out_blocks))[0]
    return final_sums[0] / GROUP, final_sums[1] / GROUP


def lamb_update(master, exp_avg, exp_sq, grad, clip_scale, learn_rate):
    bias_one = 1.0 - BETA_ONE ** STEP
    bias_two = 1.0 - BETA_TWO ** STEP
    avg_new = BETA_ONE * exp_avg + (1.0 - BETA_ONE) * clip_scale * grad
    sq_new = BETA_TWO * exp_sq + (1.0 - BETA_TWO) * (clip_scale * clip_scale) * (grad * grad)
    direction = (avg_new / bias_one) / (jnp.sqrt(sq_new / bias_two) + ADAM_EPS)
    master_norm = jnp.sqrt(jnp.sum(master * master, axis=(1, 2), keepdims=True))
    dir_norm = jnp.sqrt(jnp.sum(direction * direction, axis=(1, 2), keepdims=True))
    master_new = master - learn_rate * (master_norm / dir_norm) * direction
    return master_new, avg_new, sq_new


def row_profile(key, row_count, spread):
    walk = jnp.cumsum(jax.random.normal(key, (row_count,), jnp.float32)) / (row_count ** 0.5)
    return jnp.exp(spread * (walk - jnp.mean(walk)))


def setup_inputs(seed: int = 0) -> dict:
    keys = jax.random.split(jax.random.key(seed), 24)
    row_total = TOKENS_DEV * GROUP
    init_scale = D ** -0.5
    out_scale = (GROUP / TOKENS_DEV) ** 0.5
    act_in = jax.random.normal(keys[0], (row_total, D), jnp.float32).astype(jnp.bfloat16)
    grad_out = (jax.random.normal(keys[1], (row_total, D), jnp.float32) * out_scale).astype(jnp.bfloat16)
    prof_up = jnp.stack([row_profile(keys[2], D, 0.7), row_profile(keys[3], D, 0.7)])[:, :, None]
    prof_down = jnp.stack([row_profile(keys[4], FF, 0.7), row_profile(keys[5], FF, 0.7)])[:, :, None]
    base_up = jax.random.normal(keys[6], (2, D, FF), jnp.float32) * init_scale * prof_up
    base_down = jax.random.normal(keys[7], (2, FF, D), jnp.float32) * init_scale * prof_down
    w_up = base_up.astype(jnp.bfloat16)
    w_down = base_down.astype(jnp.bfloat16)
    master_up = base_up + 0.02 * init_scale * prof_up * jax.random.normal(keys[8], (2, D, FF), jnp.float32)
    master_down = base_down + 0.02 * init_scale * prof_down * jax.random.normal(keys[9], (2, FF, D), jnp.float32)
    grad_up, grad_down = full_grads(act_in, grad_out, w_up, w_down)
    grad_norm = jnp.sqrt(jnp.sum(grad_up * grad_up) + jnp.sum(grad_down * grad_down))
    clip_norm = jax.random.uniform(keys[10], (), jnp.float32, 0.3, 0.7) * grad_norm
    clip_scale = clip_norm / (grad_norm + NORM_EPS)
    step_up = clip_scale * jnp.sqrt(jnp.mean(grad_up * grad_up, axis=(1, 2), keepdims=True))
    step_down = clip_scale * jnp.sqrt(jnp.mean(grad_down * grad_down, axis=(1, 2), keepdims=True))
    exp_avg_up = 0.1 * step_up * jax.random.normal(keys[11], (2, D, FF), jnp.float32)
    exp_avg_down = 0.1 * step_down * jax.random.normal(keys[12], (2, FF, D), jnp.float32)
    sq_prof_up = jnp.stack([row_profile(keys[13], D, 1.5), row_profile(keys[14], D, 1.5)])[:, :, None]
    sq_prof_down = jnp.stack([row_profile(keys[15], FF, 1.5), row_profile(keys[16], FF, 1.5)])[:, :, None]
    exp_sq_up = 0.05 * step_up * step_up * sq_prof_up * jax.random.uniform(keys[17], (2, D, FF), jnp.float32, 0.5, 1.5)
    exp_sq_down = 0.05 * step_down * step_down * sq_prof_down * jax.random.uniform(keys[18], (2, FF, D), jnp.float32, 0.5, 1.5)
    learn_rate = jax.random.uniform(keys[19], (), jnp.float32, 0.08, 0.16)
    return {"act_in": act_in, "grad_out": grad_out, "w_up": w_up, "w_down": w_down, "master_up": master_up, "master_down": master_down, "exp_avg_up": exp_avg_up, "exp_avg_down": exp_avg_down, "exp_sq_up": exp_sq_up, "exp_sq_down": exp_sq_down, "learn_rate": learn_rate, "clip_norm": clip_norm}


def reference(act_in, grad_out, w_up, w_down, master_up, master_down, exp_avg_up, exp_avg_down, exp_sq_up, exp_sq_down, learn_rate, clip_norm):
    grad_up, grad_down = full_grads(act_in, grad_out, w_up, w_down)
    grad_norm = jnp.sqrt(jnp.sum(grad_up * grad_up) + jnp.sum(grad_down * grad_down))
    clip_scale = jnp.minimum(1.0, clip_norm / (grad_norm + NORM_EPS))
    master_up_out, avg_up, sq_up = lamb_update(master_up, exp_avg_up, exp_sq_up, grad_up, clip_scale, learn_rate)
    master_down_out, avg_down, sq_down = lamb_update(master_down, exp_avg_down, exp_sq_down, grad_down, clip_scale, learn_rate)
    return (master_up_out.astype(jnp.bfloat16), master_down_out.astype(jnp.bfloat16), master_up_out, master_down_out, avg_up, avg_down, sq_up, sq_down, grad_norm)
```

```python
import functools

import jax
import jax.numpy as jnp
from jax import lax
from jax.experimental import pallas as pl
from jax.experimental.pallas import tpu as pltpu
from jax.sharding import PartitionSpec as P

STEP = 10
BETA_ONE = 0.9
BETA_TWO = 0.95
ADAM_EPS = 1e-8
NORM_EPS = 1e-6
INV_SQRT_TWO = 0.7071067811865476
INV_SQRT_TWO_PI = 0.3989422804014327

GROUP = 16
TOKENS = 4096
D = 896
FF = 4864
TILE = 256
STEPS = FF // TILE
UP_ROWS = D // GROUP
DOWN_ROWS = FF // GROUP
DOWN_UNIT = DOWN_ROWS // STEPS
LAG = 2
DRAIN = 1 + 3 * LAG
SLOTS = LAG + 3
SUM_SLOTS = 3 * LAG
BLOCK = 512
MESH = pl.DeviceIdType.MESH
F32 = jnp.float32
BF16 = jnp.bfloat16


def gelu_parts(pre_act):
    normal_cdf = 0.5 * (1.0 + lax.erf(pre_act * INV_SQRT_TWO))
    normal_pdf = jnp.exp(-0.5 * pre_act * pre_act) * INV_SQRT_TWO_PI
    return pre_act * normal_cdf, normal_cdf + pre_act * normal_pdf


def dot_last(left, right):
    return lax.dot_general(left, right, (((1,), (1,)), ((), ())), preferred_element_type=F32)


def greet(devices):
    barrier = pltpu.get_barrier_semaphore()
    for device in devices:
        pl.semaphore_signal(barrier, inc=1, device_id=(device,), device_id_type=MESH)
    pl.semaphore_wait(barrier, len(devices))


class ReduceScatter:
    def __init__(self, phase, gbuf, rc, sums, r1, r2, r3, send, recv):
        self.phase = phase
        self.gbuf, self.rc, self.sums, self.landed = gbuf, rc, sums, (r1, r2, r3)
        self.send, self.recv = send, recv
        self.me = lax.axis_index("data")
        self.core = lax.rem(self.me, 2)
        self.chip = self.me // 2

    def stride_bit(self, unit, stage):
        axis = lax.rem(unit + self.phase + (0, 2, 1)[stage - 1], 3)
        stride = 1 + axis + axis * (axis - 1) // 2
        return stride, lax.rem(self.chip // stride, 2)

    def copy(self, stage, unit):
        if stage == 0:
            slot = lax.rem(unit, 2)
            src, dst = self.gbuf.at[slot, :, 1 - self.core], self.rc.at[slot]
            device = self.me + 1 - 2 * self.core
        else:
            slot = lax.rem(unit, SLOTS)
            count = 8 >> stage
            src = self.sums.at[lax.rem(unit, SUM_SLOTS), pl.ds(count, count)]
            dst = self.landed[stage - 1].at[slot]
            stride, bit = self.stride_bit(unit, stage)
            device = self.me + 2 * stride * (1 - 2 * bit)
        return pltpu.make_async_remote_copy(src_ref=src, dst_ref=dst, send_sem=self.send.at[stage, slot], recv_sem=self.recv.at[stage, slot], device_id=(device,), device_id_type=MESH)

    def finish(self, stage, unit):
        self.copy(stage, unit).wait()
        held = lax.rem(unit, SUM_SLOTS)
        if stage == 0:
            slot = lax.rem(unit, 2)
            parts = [self.stride_bit(unit, s) for s in (1, 2, 3)]
            for pos in range(8):
                chip = 0
                for (stride, bit), flip in zip(parts, (pos // 4, pos // 2 % 2, pos % 2)):
                    chip = chip + (1 - bit if flip else bit) * stride
                self.sums[held, pos] = self.gbuf[slot, chip, self.core] + self.rc[slot, chip]
        elif stage < 3:
            count = 8 >> stage
            slot = lax.rem(unit, SLOTS)
            for pos in range(count):
                self.sums[held, pos] = self.sums[held, pos] + self.landed[stage - 1][slot, pos]
        else:
            return self.sums[held, 0] + self.landed[2][lax.rem(unit, SLOTS), 0]


def within(unit):
    return jnp.logical_and(unit >= 0, unit < STEPS)


def backward_kernel(has_dx, *refs):
    if has_dx:
        z_ref, dy_ref, wd_ref, left_ref, gd_ref, wu_ref, up_ref, down_ref, dx_ref = refs[:9]
        qbuf, acc, stage_buf = refs[9:12]
        rest = refs[12:]
    else:
        z_ref, dy_ref, wd_ref, left_ref, gd_ref, up_ref, down_ref = refs[:7]
        qbuf = refs[7]
        rest = refs[8:]
    up = ReduceScatter(0, *rest[0:8])
    down = ReduceScatter(1, *rest[8:16])
    load_sem, out_sem = rest[16:18]
    step = pl.program_id(0)

    def load(unit):
        slot = lax.rem(unit, 2)
        return pltpu.make_async_copy(gd_ref.at[:, :, pl.ds(pl.multiple_of(unit * DOWN_UNIT, DOWN_UNIT), DOWN_UNIT)], down.gbuf.at[slot], load_sem.at[slot])

    @pl.when(step == 0)
    def _():
        me, core, chip = up.me, up.core, up.chip
        greet([me + 1 - 2 * core] + [me + 2 * s * (1 - 2 * lax.rem(chip // s, 2)) for s in (1, 2, 4)])
        load(0).start()
        if has_dx:
            acc[...] = jnp.zeros_like(acc)

    @pl.when(step < STEPS)
    def _():
        def block(index, carry):
            rows = pl.ds(pl.multiple_of(index * BLOCK, BLOCK), BLOCK)
            slope = gelu_parts(z_ref[rows, :])[1]
            grad = (dot_last(dy_ref[rows, :], wd_ref[...]) * slope).astype(BF16)
            qbuf[rows, :] = grad
            if has_dx:
                acc[rows, :] += dot_last(grad, wu_ref[...])
            return carry

        lax.fori_loop(0, TOKENS // BLOCK, block, 0)
        tile = jnp.dot(left_ref[...], qbuf[...], preferred_element_type=F32)
        slot = lax.rem(step, 2)
        for i in range(GROUP):
            up.gbuf[slot, i // 2, i % 2] = tile[i * UP_ROWS:(i + 1) * UP_ROWS, :]

    @pl.when(within(step - DRAIN))
    def _():
        unit = step - DRAIN
        up_ref[:, pl.ds(pl.multiple_of(unit * TILE, TILE), TILE)] = up.finish(3, unit)
        down_ref[pl.ds(pl.multiple_of(unit * DOWN_UNIT, DOWN_UNIT), DOWN_UNIT), :] = down.finish(3, unit)

    for stage in (2, 1, 0):
        unit = step - 1 - stage * LAG

        @pl.when(within(unit))
        def _():
            for ring in (up, down):
                ring.finish(stage, unit)
                ring.copy(stage + 1, unit).start()

    @pl.when(step < STEPS - 1)
    def _():
        load(step + 1).start()

    @pl.when(step < STEPS)
    def _():
        up.copy(0, step).start()
        load(step).wait()
        down.copy(0, step).start()

    if has_dx:
        @pl.when(step == STEPS - 1)
        def _():
            def flush(index, carry):
                rows = pl.ds(pl.multiple_of(index * BLOCK, BLOCK), BLOCK)
                stage_buf[...] = acc[rows, :].astype(BF16)
                out = pltpu.make_async_copy(stage_buf, dx_ref.at[rows, :], out_sem)
                out.start()
                out.wait()
                return carry

            lax.fori_loop(0, TOKENS // BLOCK, flush, 0)


def ring_scratch(rows, columns):
    block = (rows, columns)
    return [
        pltpu.VMEM((2, 8, 2) + block, F32),
        pltpu.VMEM((2, 8) + block, F32),
        pltpu.VMEM((SUM_SLOTS, 8) + block, F32),
        pltpu.VMEM((SLOTS, 4) + block, F32),
        pltpu.VMEM((SLOTS, 2) + block, F32),
        pltpu.VMEM((SLOTS, 1) + block, F32),
        pltpu.SemaphoreType.DMA((4, SLOTS)),
        pltpu.SemaphoreType.DMA((4, SLOTS)),
    ]


def backward_block(pre_act, grad, w_down, left, grad_down, w_up, collective_id):
    has_dx = w_up is not None
    last = STEPS - 1
    whole = pl.Buffered(buffer_count=1)
    in_specs = [
        pl.BlockSpec((TOKENS, TILE), lambda s: (0, jnp.minimum(s, last))),
        pl.BlockSpec((TOKENS, D), lambda s: (0, 0), pipeline_mode=whole),
        pl.BlockSpec((TILE, D), lambda s: (jnp.minimum(s, last), 0)),
        pl.BlockSpec((D, TOKENS), lambda s: (0, 0), pipeline_mode=whole),
        pl.BlockSpec(memory_space=pl.ANY),
    ]
    args = [pre_act, grad, w_down, left, grad_down.reshape(8, 2, DOWN_ROWS, D)]
    out_shape = [jax.ShapeDtypeStruct((UP_ROWS, FF), F32), jax.ShapeDtypeStruct((DOWN_ROWS, D), F32)]
    out_specs = [pl.BlockSpec((UP_ROWS, FF), lambda s: (0, 0)), pl.BlockSpec((DOWN_ROWS, D), lambda s: (0, 0))]
    scratch = [pltpu.VMEM((TOKENS, TILE), BF16)]
    if has_dx:
        in_specs.append(pl.BlockSpec((D, TILE), lambda s: (0, jnp.minimum(s, last))))
        args.append(w_up)
        out_shape.append(jax.ShapeDtypeStruct((TOKENS, D), BF16))
        out_specs.append(pl.BlockSpec(memory_space=pl.ANY))
        scratch += [pltpu.VMEM((TOKENS, D), F32), pltpu.VMEM((BLOCK, D), BF16)]
    scratch += ring_scratch(UP_ROWS, TILE) + ring_scratch(DOWN_UNIT, D)
    scratch += [pltpu.SemaphoreType.DMA((2,)), pltpu.SemaphoreType.DMA]
    return pl.pallas_call(
        functools.partial(backward_kernel, has_dx),
        grid=(STEPS + DRAIN,),
        in_specs=in_specs,
        out_specs=out_specs,
        out_shape=out_shape,
        scratch_shapes=scratch,
        compiler_params=pltpu.CompilerParams(collective_id=collective_id, has_side_effects=True, vmem_limit_bytes=67043328, dimension_semantics=("arbitrary",)),
        cost_estimate=pl.CostEstimate(flops=(6 if has_dx else 4) * TOKENS * D * FF, bytes_accessed=150 * 2**20, transcendentals=2 * TOKENS * FF),
    )(*args)


COLUMN_PARTS = ((0, 1664), (1664, 1664), (3328, 1536))
ROW_PARTS = ((0, 112), (112, 96), (208, 96))
ORDERS = ((2, 1, 0), (1, 0, 2), (0, 2, 1))
CHUNKS = 12


def tail_kernel(scalars, g1, g2, g3, g4, master_up, master_down, avg_up, avg_down, sq_up, sq_down, w_up_out, w_down_out, master_up_out, master_down_out, avg_up_out, avg_down_out, sq_up_out, sq_down_out, norm_out, send_up, send_down, dir_up, dir_down, mine, stats, stat_send, stat_recv, send_sem, recv_sem, own_sem):
    me = lax.axis_index("data")
    core = lax.rem(me, 2)
    coords = (me // 8, lax.rem(me // 4, 2), lax.rem(me // 2, 2))
    sibling = me + 1 - 2 * core
    others = [lax.rem(me + k, GROUP) for k in range(1, GROUP)]
    greet(others)

    def share(turn, row):
        mine[turn] = row
        copies = []
        for k, device in enumerate(others):
            copies.append(pltpu.make_async_remote_copy(src_ref=mine.at[turn], dst_ref=stats.at[turn, me], send_sem=stat_send.at[turn, k], recv_sem=stat_recv.at[turn, me], device_id=(device,), device_id_type=MESH))
            copies[-1].start()
        stats[turn, me] = row
        for k, device in enumerate(others):
            copies[k].wait_send()
            pltpu.make_async_remote_copy(src_ref=mine.at[turn], dst_ref=stats.at[turn, device], send_sem=stat_send.at[turn, k], recv_sem=stat_recv.at[turn, device], device_id=(device,), device_id_type=MESH).wait_recv()
        return jnp.sum(stats[turn], axis=0)

    def sum_square(values):
        return jnp.sum(values * values)

    grads = ((g1, g3), (g2, g4))
    scale = 1.0 / GROUP
    local = sum_square(g1[...] * scale) + sum_square(g3[...] * scale) + sum_square(g2[...] * scale) + sum_square(g4[...] * scale)
    total = share(0, jnp.full((8, 128), local, F32))
    norm = jnp.sqrt(total)
    clip = jnp.minimum(1.0, scalars[1] / (norm + NORM_EPS))
    norm_out[...] = norm
    clip = clip[0:1, 0:1]
    bias_one = 1.0 - BETA_ONE ** STEP
    bias_two = 1.0 - BETA_TWO ** STEP
    lane = lax.broadcasted_iota(jnp.int32, (8, 128), 1)
    row = jnp.zeros((8, 128), F32)
    families = ((master_up, avg_up, sq_up, avg_up_out, sq_up_out, dir_up), (master_down, avg_down, sq_down, avg_down_out, sq_down_out, dir_down))
    for f, (master, avg, sq, avg_out, sq_out, direction) in enumerate(families):
        for k in range(2):
            g = grads[f][k][...] * scale
            avg_new = BETA_ONE * avg[k] + (1.0 - BETA_ONE) * clip * g
            sq_new = BETA_TWO * sq[k] + (1.0 - BETA_TWO) * (clip * clip) * (g * g)
            u = (avg_new / bias_one) / (jnp.sqrt(sq_new / bias_two) + ADAM_EPS)
            avg_out[k] = avg_new
            sq_out[k] = sq_new
            direction[k] = u
            row = row + jnp.where(lane == 2 * f + k, sum_square(master[k]), 0.0) + jnp.where(lane == 4 + 2 * f + k, sum_square(u), 0.0)
    totals = share(1, row)

    def out_view(chunk, picks, flipped=None):
        index = []
        for axis in range(3):
            if axis in picks:
                index.append(slice(None))
            elif axis == flipped:
                index.append(1 - coords[axis])
            else:
                index.append(coords[axis])
        family, k, (start, size) = chunk
        if family == 0:
            return w_up_out.at[(k, *index, core, slice(None), pl.ds(start, size))]
        return w_down_out.at[(k, *index, core, pl.ds(start, size), slice(None))]

    def neighbour(axis):
        stride = (8, 4, 2)[axis]
        return me + stride * (1 - 2 * coords[axis])

    def remote(n, kind, src, dst, device):
        return pltpu.make_async_remote_copy(src_ref=src, dst_ref=dst, send_sem=send_sem.at[n, kind], recv_sem=recv_sem.at[n, kind], device_id=(device,), device_id_type=MESH)

    chunks = []
    for f, parts in enumerate((COLUMN_PARTS, ROW_PARTS)):
        for k in range(2):
            chunks += [(f, k, part) for part in parts]
    order = [ORDERS[n % 3] for n in range(CHUNKS)]
    pending = []
    rounds = [[], [], []]
    locals_ = []
    for f, (master, master_out, direction, send) in enumerate(((master_up, master_up_out, dir_up, send_up), (master_down, master_down_out, dir_down, send_down))):
        for k in range(2):
            i = 2 * f + k
            ratio = jnp.sqrt(totals[0:1, i:i + 1]) / jnp.sqrt(totals[0:1, 4 + i:5 + i])
            new = master[k] - scalars[0] * ratio * direction[k]
            master_out[k] = new
            send[k] = new.astype(BF16)
            for part in range(3):
                n = 3 * i + part
                start, size = chunks[n][2]
                if f == 0:
                    src = send.at[k, :, pl.ds(start, size)]
                else:
                    src = send.at[k, pl.ds(start, size), :]
                dst = out_view(chunks[n], ())
                rounds[0].append(remote(n, 0, src, dst, neighbour(order[n][0])))
                rounds[0][-1].start()
                pending.append(remote(n, 3, src, dst, sibling))
                pending[-1].start()
                locals_.append(pltpu.make_async_copy(src, dst, own_sem.at[n]))
                locals_[-1].start()
    for turn in range(3):
        for n in range(CHUNKS):
            first, second, third = order[n]
            if turn == 0:
                locals_[n].wait()
            rounds[turn][n].wait()
            gathered = order[n][:turn]
            view = out_view(chunks[n], gathered, order[n][turn])
            pending.append(remote(n, 4 + turn, view, view, sibling))
            pending[-1].start()
            if turn < 2:
                view = out_view(chunks[n], order[n][:turn + 1])
                rounds[turn + 1].append(remote(n, turn + 1, view, view, neighbour(order[n][turn + 1])))
                rounds[turn + 1][-1].start()
    for copy in pending:
        copy.wait()


def tail(scalars, grads, states):
    vmem = pl.BlockSpec(memory_space=pltpu.VMEM)
    any_space = pl.BlockSpec(memory_space=pl.ANY)
    up, down = (2, UP_ROWS, FF), (2, DOWN_ROWS, D)
    shape = jax.ShapeDtypeStruct
    return pl.pallas_call(
        tail_kernel,
        in_specs=[pl.BlockSpec(memory_space=pltpu.SMEM)] + [vmem] * 10,
        out_specs=[any_space] * 2 + [vmem] * 7,
        out_shape=[
            shape((2, 2, 2, 2, 2, UP_ROWS, FF), BF16),
            shape((2, 2, 2, 2, 2, DOWN_ROWS, D), BF16),
            shape(up, F32), shape(down, F32), shape(up, F32), shape(down, F32), shape(up, F32), shape(down, F32),
            shape((8, 128), F32),
        ],
        scratch_shapes=[
            pltpu.VMEM(up, BF16), pltpu.VMEM(down, BF16), pltpu.VMEM(up, F32), pltpu.VMEM(down, F32),
            pltpu.VMEM((2, 8, 128), F32), pltpu.VMEM((2, GROUP, 8, 128), F32),
            pltpu.SemaphoreType.DMA((2, GROUP)), pltpu.SemaphoreType.DMA((2, GROUP)),
            pltpu.SemaphoreType.DMA((CHUNKS, 7)), pltpu.SemaphoreType.DMA((CHUNKS, 7)), pltpu.SemaphoreType.DMA((CHUNKS,)),
        ],
        compiler_params=pltpu.CompilerParams(collective_id=3, has_side_effects=True, vmem_limit_bytes=67043328),
    )(scalars, *grads, *states)


def solution(mesh):
    batch_rows = P("data", None)
    state_rows = P(None, "data", None)
    replicated = P()

    def device_step(act_in, grad_out, w_up, w_down, master_up, master_down, exp_avg_up, exp_avg_down, exp_sq_up, exp_sq_down, learn_rate, clip_norm):
        z_one = jnp.dot(act_in, w_up[0], preferred_element_type=F32)
        act_one = gelu_parts(z_one)[0].astype(BF16)
        hidden = jnp.dot(act_one, w_down[0], preferred_element_type=F32).astype(BF16)
        z_three = jnp.dot(hidden, w_up[1], preferred_element_type=F32)
        act_three = gelu_parts(z_three)[0].astype(BF16)
        g_four = jnp.dot(act_three.T, grad_out, preferred_element_type=F32)
        shard_three, shard_four, d_hidden = backward_block(z_three, grad_out, w_down[1], hidden.T, g_four, w_up[1], 1)
        g_two = jnp.dot(act_one.T, d_hidden, preferred_element_type=F32)
        shard_one, shard_two = backward_block(z_one, d_hidden, w_down[0], act_in.T, g_two, None, 2)
        scalars = jnp.stack([learn_rate, clip_norm])
        outs = tail(scalars, (shard_one, shard_two, shard_three, shard_four), (master_up, master_down, exp_avg_up, exp_avg_down, exp_sq_up, exp_sq_down))
        new_w_up = outs[0].reshape(2, D, FF)
        new_w_down = outs[1].reshape(2, FF, D)
        return (new_w_up, new_w_down, *outs[2:8], outs[8][0, 0])

    return jax.shard_map(device_step, mesh=mesh, in_specs=(batch_rows, batch_rows, replicated, replicated, state_rows, state_rows, state_rows, state_rows, state_rows, state_rows, replicated, replicated), out_specs=(replicated, replicated, state_rows, state_rows, state_rows, state_rows, state_rows, state_rows, replicated), check_vma=False)
```

```python
import functools

import jax
import jax.numpy as jnp
from jax import lax
from jax.experimental import pallas as pl
from jax.experimental.pallas import tpu as pltpu
from jax.sharding import PartitionSpec as P

STEP = 10
BETA_ONE = 0.9
BETA_TWO = 0.95
ADAM_EPS = 1e-8
NORM_EPS = 1e-6
INV_SQRT_TWO = 0.7071067811865476
INV_SQRT_TWO_PI = 0.3989422804014327

GROUP = 16
TOKENS = 4096
D = 896
FF = 4864
TILE = 256
STEPS = FF // TILE
UP_ROWS = D // GROUP
DOWN_ROWS = FF // GROUP
DOWN_UNIT = DOWN_ROWS // STEPS
LAG = 2
DRAIN = 1 + 3 * LAG
SLOTS = LAG + 3
SUM_SLOTS = 3 * LAG
BLOCK = 512
MESH = pl.DeviceIdType.MESH
F32 = jnp.float32
BF16 = jnp.bfloat16


def gelu_parts(pre_act):
    normal_cdf = 0.5 * (1.0 + lax.erf(pre_act * INV_SQRT_TWO))
    normal_pdf = jnp.exp(-0.5 * pre_act * pre_act) * INV_SQRT_TWO_PI
    return pre_act * normal_cdf, normal_cdf + pre_act * normal_pdf


def dot_last(left, right):
    return lax.dot_general(left, right, (((1,), (1,)), ((), ())), preferred_element_type=F32)


def greet(devices):
    barrier = pltpu.get_barrier_semaphore()
    for device in devices:
        pl.semaphore_signal(barrier, inc=1, device_id=(device,), device_id_type=MESH)
    pl.semaphore_wait(barrier, len(devices))


class ReduceScatter:
    def __init__(self, phase, gbuf, rc, sums, r1, r2, r3, send, recv):
        self.phase = phase
        self.gbuf, self.rc, self.sums, self.landed = gbuf, rc, sums, (r1, r2, r3)
        self.send, self.recv = send, recv
        self.me = lax.axis_index("data")
        self.core = lax.rem(self.me, 2)
        self.chip = self.me // 2

    def stride_bit(self, unit, stage):
        axis = lax.rem(unit + self.phase + (0, 2, 1)[stage - 1], 3)
        stride = 1 + axis + axis * (axis - 1) // 2
        return stride, lax.rem(self.chip // stride, 2)

    def copy(self, stage, unit):
        if stage == 0:
            slot = lax.rem(unit, 2)
            src, dst = self.gbuf.at[slot, :, 1 - self.core], self.rc.at[slot]
            device = self.me + 1 - 2 * self.core
        else:
            slot = lax.rem(unit, SLOTS)
            count = 8 >> stage
            src = self.sums.at[lax.rem(unit, SUM_SLOTS), pl.ds(count, count)]
            dst = self.landed[stage - 1].at[slot]
            stride, bit = self.stride_bit(unit, stage)
            device = self.me + 2 * stride * (1 - 2 * bit)
        return pltpu.make_async_remote_copy(src_ref=src, dst_ref=dst, send_sem=self.send.at[stage, slot], recv_sem=self.recv.at[stage, slot], device_id=(device,), device_id_type=MESH)

    def finish(self, stage, unit):
        self.copy(stage, unit).wait()
        held = lax.rem(unit, SUM_SLOTS)
        if stage == 0:
            slot = lax.rem(unit, 2)
            parts = [self.stride_bit(unit, s) for s in (1, 2, 3)]
            for pos in range(8):
                chip = 0
                for (stride, bit), flip in zip(parts, (pos // 4, pos // 2 % 2, pos % 2)):
                    chip = chip + (1 - bit if flip else bit) * stride
                self.sums[held, pos] = self.gbuf[slot, chip, self.core] + self.rc[slot, chip]
        elif stage < 3:
            count = 8 >> stage
            slot = lax.rem(unit, SLOTS)
            for pos in range(count):
                self.sums[held, pos] = self.sums[held, pos] + self.landed[stage - 1][slot, pos]
        else:
            return self.sums[held, 0] + self.landed[2][lax.rem(unit, SLOTS), 0]


def within(unit):
    return jnp.logical_and(unit >= 0, unit < STEPS)


def backward_kernel(has_dx, *refs):
    if has_dx:
        z_ref, dy_ref, wd_ref, left_ref, gd_ref, wu_ref, up_ref, down_ref, dx_ref = refs[:9]
        qbuf, acc, stage_buf = refs[9:12]
        rest = refs[12:]
    else:
        z_ref, dy_ref, wd_ref, left_ref, gd_ref, up_ref, down_ref = refs[:7]
        qbuf = refs[7]
        rest = refs[8:]
    up = ReduceScatter(0, *rest[0:8])
    down = ReduceScatter(1, *rest[8:16])
    load_sem, out_sem = rest[16:18]
    step = pl.program_id(0)

    def load(unit):
        slot = lax.rem(unit, 2)
        return pltpu.make_async_copy(gd_ref.at[:, :, pl.ds(pl.multiple_of(unit * DOWN_UNIT, DOWN_UNIT), DOWN_UNIT)], down.gbuf.at[slot], load_sem.at[slot])

    @pl.when(step == 0)
    def _():
        me, core, chip = up.me, up.core, up.chip
        greet([me + 1 - 2 * core] + [me + 2 * s * (1 - 2 * lax.rem(chip // s, 2)) for s in (1, 2, 4)])
        load(0).start()
        if has_dx:
            acc[...] = jnp.zeros_like(acc)

    @pl.when(step < STEPS)
    def _():
        def block(index, carry):
            rows = pl.ds(pl.multiple_of(index * BLOCK, BLOCK), BLOCK)
            slope = gelu_parts(z_ref[rows, :])[1]
            grad = (dot_last(dy_ref[rows, :], wd_ref[...]) * slope).astype(BF16)
            qbuf[rows, :] = grad
            if has_dx:
                acc[rows, :] += dot_last(grad, wu_ref[...])
            return carry

        lax.fori_loop(0, TOKENS // BLOCK, block, 0, unroll=TOKENS // BLOCK)
        tile = jnp.dot(left_ref[...], qbuf[...], preferred_element_type=F32)
        slot = lax.rem(step, 2)
        for i in range(GROUP):
            up.gbuf[slot, i // 2, i % 2] = tile[i * UP_ROWS:(i + 1) * UP_ROWS, :]

    @pl.when(within(step - DRAIN))
    def _():
        unit = step - DRAIN
        up_ref[:, pl.ds(pl.multiple_of(unit * TILE, TILE), TILE)] = up.finish(3, unit)
        down_ref[pl.ds(pl.multiple_of(unit * DOWN_UNIT, DOWN_UNIT), DOWN_UNIT), :] = down.finish(3, unit)

    for stage in (2, 1, 0):
        unit = step - 1 - stage * LAG

        @pl.when(within(unit))
        def _():
            for ring in (up, down):
                ring.finish(stage, unit)
                ring.copy(stage + 1, unit).start()

    @pl.when(step < STEPS - 1)
    def _():
        load(step + 1).start()

    @pl.when(step < STEPS)
    def _():
        up.copy(0, step).start()
        load(step).wait()
        down.copy(0, step).start()

    if has_dx:
        @pl.when(step == STEPS - 1)
        def _():
            def flush(index, carry):
                rows = pl.ds(pl.multiple_of(index * BLOCK, BLOCK), BLOCK)
                stage_buf[...] = acc[rows, :].astype(BF16)
                out = pltpu.make_async_copy(stage_buf, dx_ref.at[rows, :], out_sem)
                out.start()
                out.wait()
                return carry

            lax.fori_loop(0, TOKENS // BLOCK, flush, 0)


def ring_scratch(rows, columns):
    block = (rows, columns)
    return [
        pltpu.VMEM((2, 8, 2) + block, F32),
        pltpu.VMEM((2, 8) + block, F32),
        pltpu.VMEM((SUM_SLOTS, 8) + block, F32),
        pltpu.VMEM((SLOTS, 4) + block, F32),
        pltpu.VMEM((SLOTS, 2) + block, F32),
        pltpu.VMEM((SLOTS, 1) + block, F32),
        pltpu.SemaphoreType.DMA((4, SLOTS)),
        pltpu.SemaphoreType.DMA((4, SLOTS)),
    ]


def backward_block(pre_act, grad, w_down, left, grad_down, w_up, layer, collective_id):
    has_dx = w_up is not None
    last = STEPS - 1
    whole = pl.Buffered(buffer_count=1)
    in_specs = [
        pl.BlockSpec((TOKENS, TILE), lambda s: (0, jnp.minimum(s, last))),
        pl.BlockSpec((TOKENS, D), lambda s: (0, 0), pipeline_mode=whole),
        pl.BlockSpec((None, TILE, D), lambda s: (layer, jnp.minimum(s, last), 0)),
        pl.BlockSpec((D, TOKENS), lambda s: (0, 0), pipeline_mode=whole),
        pl.BlockSpec(memory_space=pl.ANY),
    ]
    args = [pre_act, grad, w_down, left, grad_down.reshape(8, 2, DOWN_ROWS, D)]
    out_shape = [jax.ShapeDtypeStruct((UP_ROWS, FF), F32), jax.ShapeDtypeStruct((DOWN_ROWS, D), F32)]
    out_specs = [pl.BlockSpec((UP_ROWS, FF), lambda s: (0, 0)), pl.BlockSpec((DOWN_ROWS, D), lambda s: (0, 0))]
    scratch = [pltpu.VMEM((TOKENS, TILE), BF16)]
    if has_dx:
        in_specs.append(pl.BlockSpec((None, D, TILE), lambda s: (layer, 0, jnp.minimum(s, last))))
        args.append(w_up)
        out_shape.append(jax.ShapeDtypeStruct((TOKENS, D), BF16))
        out_specs.append(pl.BlockSpec(memory_space=pl.ANY))
        scratch += [pltpu.VMEM((TOKENS, D), F32), pltpu.VMEM((BLOCK, D), BF16)]
    scratch += ring_scratch(UP_ROWS, TILE) + ring_scratch(DOWN_UNIT, D)
    scratch += [pltpu.SemaphoreType.DMA((2,)), pltpu.SemaphoreType.DMA]
    return pl.pallas_call(
        functools.partial(backward_kernel, has_dx),
        grid=(STEPS + DRAIN,),
        in_specs=in_specs,
        out_specs=out_specs,
        out_shape=out_shape,
        scratch_shapes=scratch,
        compiler_params=pltpu.CompilerParams(collective_id=collective_id, has_side_effects=True, vmem_limit_bytes=67043328, dimension_semantics=("arbitrary",)),
        cost_estimate=pl.CostEstimate(flops=(6 if has_dx else 4) * TOKENS * D * FF, bytes_accessed=150 * 2**20, transcendentals=2 * TOKENS * FF),
    )(*args)


COLUMN_PARTS = ((0, 1664), (1664, 1664), (3328, 1536))
ROW_PARTS = ((0, 112), (112, 96), (208, 96))
ORDERS = ((2, 1, 0), (1, 0, 2), (0, 2, 1))
CHUNKS = 12


def tail_kernel(scalars, g1, g2, g3, g4, master_up, master_down, avg_up, avg_down, sq_up, sq_down, w_up_out, w_down_out, master_up_out, master_down_out, avg_up_out, avg_down_out, sq_up_out, sq_down_out, norm_out, send_up, send_down, dir_up, dir_down, mine, stats, stat_send, stat_recv, send_sem, recv_sem, own_sem):
    me = lax.axis_index("data")
    core = lax.rem(me, 2)
    coords = (me // 8, lax.rem(me // 4, 2), lax.rem(me // 2, 2))
    sibling = me + 1 - 2 * core
    others = [lax.rem(me + k, GROUP) for k in range(1, GROUP)]
    greet(others)

    def share(turn, row):
        mine[turn] = row
        copies = []
        for k, device in enumerate(others):
            copies.append(pltpu.make_async_remote_copy(src_ref=mine.at[turn], dst_ref=stats.at[turn, me], send_sem=stat_send.at[turn, k], recv_sem=stat_recv.at[turn, me], device_id=(device,), device_id_type=MESH))
            copies[-1].start()
        stats[turn, me] = row
        for k, device in enumerate(others):
            copies[k].wait_send()
            pltpu.make_async_remote_copy(src_ref=mine.at[turn], dst_ref=stats.at[turn, device], send_sem=stat_send.at[turn, k], recv_sem=stat_recv.at[turn, device], device_id=(device,), device_id_type=MESH).wait_recv()
        return jnp.sum(stats[turn], axis=0)

    def sum_square(values):
        return jnp.sum(values * values)

    grads = ((g1, g3), (g2, g4))
    scale = 1.0 / GROUP
    local = sum_square(g1[...] * scale) + sum_square(g3[...] * scale) + sum_square(g2[...] * scale) + sum_square(g4[...] * scale)
    total = share(0, jnp.full((8, 128), local, F32))
    norm = jnp.sqrt(total)
    clip = jnp.minimum(1.0, scalars[1] / (norm + NORM_EPS))
    norm_out[...] = norm
    clip = clip[0:1, 0:1]
    bias_one = 1.0 - BETA_ONE ** STEP
    bias_two = 1.0 - BETA_TWO ** STEP
    lane = lax.broadcasted_iota(jnp.int32, (8, 128), 1)
    row = jnp.zeros((8, 128), F32)
    families = ((master_up, avg_up, sq_up, avg_up_out, sq_up_out, dir_up), (master_down, avg_down, sq_down, avg_down_out, sq_down_out, dir_down))
    for f, (master, avg, sq, avg_out, sq_out, direction) in enumerate(families):
        for k in range(2):
            g = grads[f][k][...] * scale
            avg_new = BETA_ONE * avg[k] + (1.0 - BETA_ONE) * clip * g
            sq_new = BETA_TWO * sq[k] + (1.0 - BETA_TWO) * (clip * clip) * (g * g)
            u = (avg_new / bias_one) / (jnp.sqrt(sq_new / bias_two) + ADAM_EPS)
            avg_out[k] = avg_new
            sq_out[k] = sq_new
            direction[k] = u
            row = row + jnp.where(lane == 2 * f + k, sum_square(master[k]), 0.0) + jnp.where(lane == 4 + 2 * f + k, sum_square(u), 0.0)
    totals = share(1, row)

    def out_view(chunk, picks, flipped=None):
        index = []
        for axis in range(3):
            if axis in picks:
                index.append(slice(None))
            elif axis == flipped:
                index.append(1 - coords[axis])
            else:
                index.append(coords[axis])
        family, k, (start, size) = chunk
        if family == 0:
            return w_up_out.at[(k, *index, core, slice(None), pl.ds(start, size))]
        return w_down_out.at[(k, *index, core, pl.ds(start, size), slice(None))]

    def neighbour(axis):
        stride = (8, 4, 2)[axis]
        return me + stride * (1 - 2 * coords[axis])

    def remote(n, kind, src, dst, device):
        return pltpu.make_async_remote_copy(src_ref=src, dst_ref=dst, send_sem=send_sem.at[n, kind], recv_sem=recv_sem.at[n, kind], device_id=(device,), device_id_type=MESH)

    chunks = []
    for f, parts in enumerate((COLUMN_PARTS, ROW_PARTS)):
        for k in range(2):
            chunks += [(f, k, part) for part in parts]
    order = [ORDERS[n % 3] for n in range(CHUNKS)]
    pending = []
    rounds = [[], [], []]
    locals_ = []
    for f, (master, master_out, direction, send) in enumerate(((master_up, master_up_out, dir_up, send_up), (master_down, master_down_out, dir_down, send_down))):
        for k in range(2):
            i = 2 * f + k
            ratio = jnp.sqrt(totals[0:1, i:i + 1]) / jnp.sqrt(totals[0:1, 4 + i:5 + i])
            new = master[k] - scalars[0] * ratio * direction[k]
            master_out[k] = new
            send[k] = new.astype(BF16)
            for part in range(3):
                n = 3 * i + part
                start, size = chunks[n][2]
                if f == 0:
                    src = send.at[k, :, pl.ds(start, size)]
                else:
                    src = send.at[k, pl.ds(start, size), :]
                dst = out_view(chunks[n], ())
                rounds[0].append(remote(n, 0, src, dst, neighbour(order[n][0])))
                rounds[0][-1].start()
                pending.append(remote(n, 3, src, dst, sibling))
                pending[-1].start()
                locals_.append(pltpu.make_async_copy(src, dst, own_sem.at[n]))
                locals_[-1].start()
    for turn in range(3):
        for n in range(CHUNKS):
            first, second, third = order[n]
            if turn == 0:
                locals_[n].wait()
            rounds[turn][n].wait()
            gathered = order[n][:turn]
            view = out_view(chunks[n], gathered, order[n][turn])
            pending.append(remote(n, 4 + turn, view, view, sibling))
            pending[-1].start()
            if turn < 2:
                view = out_view(chunks[n], order[n][:turn + 1])
                rounds[turn + 1].append(remote(n, turn + 1, view, view, neighbour(order[n][turn + 1])))
                rounds[turn + 1][-1].start()
    for copy in pending:
        copy.wait()


def tail(scalars, grads, states):
    vmem = pl.BlockSpec(memory_space=pltpu.VMEM)
    any_space = pl.BlockSpec(memory_space=pl.ANY)
    up, down = (2, UP_ROWS, FF), (2, DOWN_ROWS, D)
    shape = jax.ShapeDtypeStruct
    return pl.pallas_call(
        tail_kernel,
        in_specs=[pl.BlockSpec(memory_space=pltpu.SMEM)] + [vmem] * 10,
        out_specs=[any_space] * 2 + [vmem] * 7,
        out_shape=[
            shape((2, 2, 2, 2, 2, UP_ROWS, FF), BF16),
            shape((2, 2, 2, 2, 2, DOWN_ROWS, D), BF16),
            shape(up, F32), shape(down, F32), shape(up, F32), shape(down, F32), shape(up, F32), shape(down, F32),
            shape((8, 128), F32),
        ],
        scratch_shapes=[
            pltpu.VMEM(up, BF16), pltpu.VMEM(down, BF16), pltpu.VMEM(up, F32), pltpu.VMEM(down, F32),
            pltpu.VMEM((2, 8, 128), F32), pltpu.VMEM((2, GROUP, 8, 128), F32),
            pltpu.SemaphoreType.DMA((2, GROUP)), pltpu.SemaphoreType.DMA((2, GROUP)),
            pltpu.SemaphoreType.DMA((CHUNKS, 7)), pltpu.SemaphoreType.DMA((CHUNKS, 7)), pltpu.SemaphoreType.DMA((CHUNKS,)),
        ],
        compiler_params=pltpu.CompilerParams(collective_id=3, has_side_effects=True, vmem_limit_bytes=67043328),
    )(scalars, *grads, *states)


def solution(mesh):
    batch_rows = P("data", None)
    state_rows = P(None, "data", None)
    replicated = P()

    def device_step(act_in, grad_out, w_up, w_down, master_up, master_down, exp_avg_up, exp_avg_down, exp_sq_up, exp_sq_down, learn_rate, clip_norm):
        z_one = jnp.dot(act_in, w_up[0], preferred_element_type=F32)
        act_one = gelu_parts(z_one)[0].astype(BF16)
        hidden = jnp.dot(act_one, w_down[0], preferred_element_type=F32).astype(BF16)
        z_three = jnp.dot(hidden, w_up[1], preferred_element_type=F32)
        act_three = gelu_parts(z_three)[0].astype(BF16)
        g_four = jnp.dot(act_three.T, grad_out, preferred_element_type=F32)
        shard_three, shard_four, d_hidden = backward_block(z_three, grad_out, w_down, hidden.T, g_four, w_up, 1, 1)
        g_two = jnp.dot(act_one.T, d_hidden, preferred_element_type=F32)
        shard_one, shard_two = backward_block(z_one, d_hidden, w_down, act_in.T, g_two, None, 0, 2)
        scalars = jnp.stack([learn_rate, clip_norm])
        outs = tail(scalars, (shard_one, shard_two, shard_three, shard_four), (master_up, master_down, exp_avg_up, exp_avg_down, exp_sq_up, exp_sq_down))
        new_w_up = outs[0].reshape(2, D, FF)
        new_w_down = outs[1].reshape(2, FF, D)
        return (new_w_up, new_w_down, *outs[2:8], outs[8][0, 0])

    return jax.shard_map(device_step, mesh=mesh, in_specs=(batch_rows, batch_rows, replicated, replicated, state_rows, state_rows, state_rows, state_rows, state_rows, state_rows, replicated, replicated), out_specs=(replicated, replicated, state_rows, state_rows, state_rows, state_rows, state_rows, state_rows, replicated), check_vma=False)
```

```python
import functools

import jax
import jax.numpy as jnp
from jax import lax
from jax.experimental import pallas as pl
from jax.experimental.pallas import tpu as pltpu
from jax.sharding import PartitionSpec as P

STEP = 10
BETA_ONE = 0.9
BETA_TWO = 0.95
ADAM_EPS = 1e-8
NORM_EPS = 1e-6
INV_SQRT_TWO = 0.7071067811865476
INV_SQRT_TWO_PI = 0.3989422804014327

GROUP = 16
TOKENS = 4096
D = 896
FF = 4864
TILE = 256
STEPS = FF // TILE
UP_ROWS = D // GROUP
DOWN_ROWS = FF // GROUP
DOWN_UNIT = DOWN_ROWS // STEPS
LAG = 2
DRAIN = 1 + 3 * LAG
SLOTS = LAG + 3
SUM_SLOTS = 3 * LAG
BLOCK = 512
MESH = pl.DeviceIdType.MESH
F32 = jnp.float32
BF16 = jnp.bfloat16


def gelu_parts(pre_act):
    normal_cdf = 0.5 * (1.0 + lax.erf(pre_act * INV_SQRT_TWO))
    normal_pdf = jnp.exp(-0.5 * pre_act * pre_act) * INV_SQRT_TWO_PI
    return pre_act * normal_cdf, normal_cdf + pre_act * normal_pdf


def dot_last(left, right):
    return lax.dot_general(left, right, (((1,), (1,)), ((), ())), preferred_element_type=F32)


def greet(devices):
    barrier = pltpu.get_barrier_semaphore()
    for device in devices:
        pl.semaphore_signal(barrier, inc=1, device_id=(device,), device_id_type=MESH)
    pl.semaphore_wait(barrier, len(devices))


class ReduceScatter:
    def __init__(self, phase, gbuf, rc, sums, r1, r2, r3, send, recv):
        self.phase = phase
        self.gbuf, self.rc, self.sums, self.landed = gbuf, rc, sums, (r1, r2, r3)
        self.send, self.recv = send, recv
        self.me = lax.axis_index("data")
        self.core = lax.rem(self.me, 2)
        self.chip = self.me // 2

    def stride_bit(self, unit, stage):
        axis = lax.rem(unit + self.phase + (0, 2, 1)[stage - 1], 3)
        stride = 1 + axis + axis * (axis - 1) // 2
        return stride, lax.rem(self.chip // stride, 2)

    def copy(self, stage, unit):
        if stage == 0:
            slot = lax.rem(unit, 2)
            src, dst = self.gbuf.at[slot, :, 1 - self.core], self.rc.at[slot]
            device = self.me + 1 - 2 * self.core
        else:
            slot = lax.rem(unit, SLOTS)
            count = 8 >> stage
            src = self.sums.at[lax.rem(unit, SUM_SLOTS), pl.ds(count, count)]
            dst = self.landed[stage - 1].at[slot]
            stride, bit = self.stride_bit(unit, stage)
            device = self.me + 2 * stride * (1 - 2 * bit)
        return pltpu.make_async_remote_copy(src_ref=src, dst_ref=dst, send_sem=self.send.at[stage, slot], recv_sem=self.recv.at[stage, slot], device_id=(device,), device_id_type=MESH)

    def finish(self, stage, unit):
        self.copy(stage, unit).wait()
        held = lax.rem(unit, SUM_SLOTS)
        if stage == 0:
            slot = lax.rem(unit, 2)
            parts = [self.stride_bit(unit, s) for s in (1, 2, 3)]
            for pos in range(8):
                chip = 0
                for (stride, bit), flip in zip(parts, (pos // 4, pos // 2 % 2, pos % 2)):
                    chip = chip + (1 - bit if flip else bit) * stride
                self.sums[held, pos] = self.gbuf[slot, chip, self.core] + self.rc[slot, chip]
        elif stage < 3:
            count = 8 >> stage
            slot = lax.rem(unit, SLOTS)
            for pos in range(count):
                self.sums[held, pos] = self.sums[held, pos] + self.landed[stage - 1][slot, pos]
        else:
            return self.sums[held, 0] + self.landed[2][lax.rem(unit, SLOTS), 0]


def within(unit, count):
    return jnp.logical_and(unit >= 0, unit < count)


def advance(ring, tick, count, emit):
    @pl.when(within(tick - DRAIN, count))
    def _():
        emit(tick - DRAIN, ring.finish(3, tick - DRAIN))

    for stage in (2, 1, 0):
        unit = tick - 1 - stage * LAG

        @pl.when(within(unit, count))
        def _():
            ring.finish(stage, unit)
            ring.copy(stage + 1, unit).start()


def greet_partners(ring):
    me, core, chip = ring.me, ring.core, ring.chip
    greet([me + 1 - 2 * core] + [me + 2 * s * (1 - 2 * lax.rem(chip // s, 2)) for s in (1, 2, 4)])


def aligned(index, size):
    return pl.ds(pl.multiple_of(index * size, size), size)


def grad_tile(z_ref, dy_ref, wd_ref, qbuf, extra):
    def block(index, carry):
        rows = aligned(index, BLOCK)
        slope = gelu_parts(z_ref[rows, :])[1]
        grad = (dot_last(dy_ref[rows, :], wd_ref[...]) * slope).astype(BF16)
        qbuf[rows, :] = grad
        extra(rows, grad)
        return carry

    lax.fori_loop(0, TOKENS // BLOCK, block, 0, unroll=TOKENS // BLOCK)


def store_tile(left, qbuf, gbuf, slot):
    tile = jnp.dot(left[...], qbuf[...], preferred_element_type=F32)
    for i in range(GROUP):
        gbuf[slot, i // 2, i % 2] = tile[i * UP_ROWS:(i + 1) * UP_ROWS, :]


def second_block_kernel(z_ref, dy_ref, wd_ref, left_ref, gd_ref, wu_ref, up_ref, down_ref, dx_ref, dxt_ref, qbuf, acc, stage_buf, stage_t, *rest):
    up = ReduceScatter(0, *rest[0:8])
    down = ReduceScatter(1, *rest[8:16])
    load_sem, out_sem = rest[16:18]
    step = pl.program_id(0)

    def load(unit):
        slot = lax.rem(unit, 2)
        return pltpu.make_async_copy(gd_ref.at[:, :, aligned(unit, DOWN_UNIT)], down.gbuf.at[slot], load_sem.at[slot])

    @pl.when(step == 0)
    def _():
        greet_partners(up)
        load(0).start()
        acc[...] = jnp.zeros_like(acc)

    def add_dx(rows, grad):
        acc[rows, :] += dot_last(grad, wu_ref[...])

    @pl.when(step < STEPS)
    def _():
        grad_tile(z_ref, dy_ref, wd_ref, qbuf, add_dx)
        store_tile(left_ref, qbuf, up.gbuf, lax.rem(step, 2))

    def emit_up(unit, block):
        up_ref[:, aligned(unit, TILE)] = block

    def emit_down(unit, block):
        down_ref[aligned(unit, DOWN_UNIT), :] = block

    advance(up, step, STEPS, emit_up)
    advance(down, step, STEPS, emit_down)

    @pl.when(step < STEPS - 1)
    def _():
        load(step + 1).start()

    @pl.when(step < STEPS)
    def _():
        up.copy(0, step).start()
        load(step).wait()
        down.copy(0, step).start()

    @pl.when(step == STEPS - 1)
    def _():
        def flush(index, carry):
            rows = aligned(index, BLOCK)
            value = acc[rows, :]
            stage_buf[...] = value.astype(BF16)
            stage_t[...] = value.T.astype(BF16)
            outs = [pltpu.make_async_copy(stage_buf, dx_ref.at[rows, :], out_sem.at[0]), pltpu.make_async_copy(stage_t, dxt_ref.at[:, rows], out_sem.at[1])]
            for out in outs:
                out.start()
            for out in outs:
                out.wait()
            return carry

        lax.fori_loop(0, TOKENS // BLOCK, flush, 0)


def first_block_kernel(z_ref, dy_ref, wd_ref, dyt_ref, act_ref, x_ref, up_ref, down_ref, gd_ref, qbuf, left, stage_buf, *rest):
    up = ReduceScatter(0, *rest[0:8])
    down = ReduceScatter(1, *rest[8:16])
    load_sem, out_sem = rest[16:18]
    step = pl.program_id(0)

    def loads(unit):
        slot = lax.rem(unit, 2)
        columns, half = aligned(unit // 2, LANES), lax.rem(unit, 2) * HALF_ROWS
        copies = []
        for i in range(GROUP):
            rows = pl.ds(pl.multiple_of(i * DOWN_ROWS + half, 8), HALF_ROWS)
            copies.append(pltpu.make_async_copy(gd_ref.at[rows, columns], down.gbuf.at[slot, i // 2, i % 2], load_sem.at[slot, i]))
        return copies

    def write(index, split):
        slot = lax.rem(index, 2)
        rows = aligned(lax.rem(index, STEPS), TILE)
        if split == 0:
            return pltpu.make_async_copy(stage_buf.at[slot, :, pl.ds(0, SPLIT)], gd_ref.at[rows, pl.ds(0, SPLIT)], out_sem.at[slot])
        return pltpu.make_async_copy(stage_buf.at[slot, :, pl.ds(0, D - SPLIT)], gd_ref.at[rows, pl.ds(SPLIT, D - SPLIT)], out_sem.at[slot])

    @pl.when(step == 0)
    def _():
        greet_partners(up)

    @pl.when(step < TOKENS // TILE)
    def _():
        left[:, aligned(step, TILE)] = x_ref[...].T

    for split in (0, 1):
        @pl.when(within(step - split * STEPS, STEPS))
        def _():
            width = SPLIT if split == 0 else D - SPLIT
            part = jnp.dot(dyt_ref[pl.ds(split * SPLIT, width), :], act_ref[...], preferred_element_type=F32)
            stage_buf[lax.rem(step, 2), :, pl.ds(0, width)] = part.T

    for split in (0, 1):
        @pl.when(within(step - 1 - split * STEPS, STEPS))
        def _():
            write(step - 1, split).wait()

    for split in (0, 1):
        @pl.when(within(step - split * STEPS, STEPS))
        def _():
            write(step, split).start()

    tile = step - 2 * STEPS

    @pl.when(within(tile, STEPS))
    def _():
        grad_tile(z_ref, dy_ref, wd_ref, qbuf, lambda rows, grad: None)
        store_tile(left, qbuf, up.gbuf, lax.rem(tile, 2))

    def emit_up(unit, block):
        up_ref[:, aligned(unit, TILE)] = block

    def emit_down(unit, block):
        down_ref[pl.ds(pl.multiple_of(lax.rem(unit, 2) * HALF_ROWS, 8), HALF_ROWS), aligned(unit // 2, LANES)] = block

    early = step - FIRST_TICK
    ticking = jnp.logical_or(jnp.logical_and(early >= 0, lax.rem(early, TICK_GAP) == 0), tile >= 0)
    tick = jnp.where(tile >= 0, tile + (2 * STEPS - FIRST_TICK) // TICK_GAP, early // TICK_GAP)
    tick = jnp.where(ticking, tick, -1)

    advance(up, tile, STEPS, emit_up)
    advance(down, tick, DOWN_UNITS, emit_down)

    @pl.when(step == FIRST_TICK - 1)
    def _():
        for copy in loads(0):
            copy.start()

    @pl.when(within(tick, DOWN_UNITS - 1))
    def _():
        for copy in loads(tick + 1):
            copy.start()

    @pl.when(within(tile, STEPS))
    def _():
        up.copy(0, tile).start()

    @pl.when(within(tick, DOWN_UNITS))
    def _():
        for copy in loads(tick):
            copy.wait()
        down.copy(0, tick).start()


def ring_scratch(rows, columns):
    block = (rows, columns)
    return [
        pltpu.VMEM((2, 8, 2) + block, F32),
        pltpu.VMEM((2, 8) + block, F32),
        pltpu.VMEM((SUM_SLOTS, 8) + block, F32),
        pltpu.VMEM((SLOTS, 4) + block, F32),
        pltpu.VMEM((SLOTS, 2) + block, F32),
        pltpu.VMEM((SLOTS, 1) + block, F32),
        pltpu.SemaphoreType.DMA((4, SLOTS)),
        pltpu.SemaphoreType.DMA((4, SLOTS)),
    ]


WHOLE = pl.Buffered(buffer_count=1)
ANY = pl.BlockSpec(memory_space=pl.ANY)


def params(collective_id):
    return pltpu.CompilerParams(collective_id=collective_id, has_side_effects=True, vmem_limit_bytes=67043328, dimension_semantics=("arbitrary",))


def second_block(pre_act, grad, w_down, left, grad_down, w_up):
    last = STEPS - 1
    return pl.pallas_call(
        second_block_kernel,
        grid=(STEPS + DRAIN,),
        in_specs=[
            pl.BlockSpec((TOKENS, TILE), lambda s: (0, jnp.minimum(s, last))),
            pl.BlockSpec((TOKENS, D), lambda s: (0, 0), pipeline_mode=WHOLE),
            pl.BlockSpec((None, TILE, D), lambda s: (1, jnp.minimum(s, last), 0)),
            pl.BlockSpec((D, TOKENS), lambda s: (0, 0), pipeline_mode=WHOLE),
            ANY,
            pl.BlockSpec((None, D, TILE), lambda s: (1, 0, jnp.minimum(s, last))),
        ],
        out_specs=[pl.BlockSpec((UP_ROWS, FF), lambda s: (0, 0)), pl.BlockSpec((DOWN_ROWS, D), lambda s: (0, 0)), ANY, ANY],
        out_shape=[jax.ShapeDtypeStruct((UP_ROWS, FF), F32), jax.ShapeDtypeStruct((DOWN_ROWS, D), F32), jax.ShapeDtypeStruct((TOKENS, D), BF16), jax.ShapeDtypeStruct((D, TOKENS), BF16)],
        scratch_shapes=[pltpu.VMEM((TOKENS, TILE), BF16), pltpu.VMEM((TOKENS, D), F32), pltpu.VMEM((BLOCK, D), BF16), pltpu.VMEM((D, BLOCK), BF16)] + ring_scratch(UP_ROWS, TILE) + ring_scratch(DOWN_UNIT, D) + [pltpu.SemaphoreType.DMA((2,)), pltpu.SemaphoreType.DMA((2,))],
        compiler_params=params(1),
        cost_estimate=pl.CostEstimate(flops=6 * TOKENS * D * FF, bytes_accessed=150 * 2**20, transcendentals=2 * TOKENS * FF),
    )(pre_act, grad, w_down, left, grad_down.reshape(8, 2, DOWN_ROWS, D), w_up)


LANES = 128
HALF_ROWS = DOWN_ROWS // 2
DOWN_UNITS = 2 * D // LANES
SPLIT = 512
TICK_GAP = 4
FIRST_TICK = STEPS + 3


def first_block(pre_act, grad, w_down, grad_t, act, act_in):
    start, last = 2 * STEPS, STEPS - 1
    return pl.pallas_call(
        first_block_kernel,
        grid=(start + STEPS + DRAIN,),
        in_specs=[
            pl.BlockSpec((TOKENS, TILE), lambda s: (0, jnp.clip(s - start, 0, last))),
            pl.BlockSpec((TOKENS, D), lambda s: (0, 0), pipeline_mode=WHOLE),
            pl.BlockSpec((None, TILE, D), lambda s: (0, jnp.clip(s - start, 0, last), 0)),
            pl.BlockSpec((D, TOKENS), lambda s: (0, 0), pipeline_mode=WHOLE),
            pl.BlockSpec((TOKENS, TILE), lambda s: (0, lax.rem(jnp.minimum(s, start - 1), STEPS))),
            pl.BlockSpec((TILE, D), lambda s: (jnp.minimum(s, TOKENS // TILE - 1), 0)),
        ],
        out_specs=[pl.BlockSpec((UP_ROWS, FF), lambda s: (0, 0)), pl.BlockSpec((DOWN_ROWS, D), lambda s: (0, 0)), ANY],
        out_shape=[jax.ShapeDtypeStruct((UP_ROWS, FF), F32), jax.ShapeDtypeStruct((DOWN_ROWS, D), F32), jax.ShapeDtypeStruct((FF, D), F32)],
        scratch_shapes=[pltpu.VMEM((TOKENS, TILE), BF16), pltpu.VMEM((D, TOKENS), BF16), pltpu.VMEM((2, TILE, SPLIT), F32)] + ring_scratch(UP_ROWS, TILE) + ring_scratch(HALF_ROWS, LANES) + [pltpu.SemaphoreType.DMA((2, GROUP)), pltpu.SemaphoreType.DMA((2,))],
        compiler_params=params(2),
        cost_estimate=pl.CostEstimate(flops=6 * TOKENS * D * FF, bytes_accessed=250 * 2**20, transcendentals=2 * TOKENS * FF),
    )(pre_act, grad, w_down, grad_t, act, act_in)


COLUMN_PARTS = ((0, 1664), (1664, 1664), (3328, 1536))
ROW_PARTS = ((0, 112), (112, 96), (208, 96))
ORDERS = ((2, 1, 0), (1, 0, 2), (0, 2, 1))
CHUNKS = 12


def tail_kernel(scalars, g1, g2, g3, g4, *refs):
    states, (w_up_out, w_down_out), state_outs, norm_out = refs[:6], refs[6:8], refs[8:14], refs[14]
    send_up, send_down, dir_up, dir_down, mine, stats, stat_send, stat_recv, send_sem, recv_sem, own_sem = refs[15:26]
    held, (in_sem, out_sem) = refs[26:32], refs[32:34]
    master_up, master_down, avg_up, avg_down, sq_up, sq_down = held
    fetches = [pltpu.make_async_copy(src, dst, in_sem.at[i]) for i, (src, dst) in enumerate(zip(states, held))]
    stores = [pltpu.make_async_copy(src, dst, out_sem.at[i]) for i, (src, dst) in enumerate(zip(held, state_outs))]
    for copy in fetches:
        copy.start()
    me = lax.axis_index("data")
    core = lax.rem(me, 2)
    coords = (me // 8, lax.rem(me // 4, 2), lax.rem(me // 2, 2))
    sibling = me + 1 - 2 * core
    others = [lax.rem(me + k, GROUP) for k in range(1, GROUP)]
    greet(others)

    def share(turn, row):
        mine[turn] = row
        copies = []
        for k, device in enumerate(others):
            copies.append(pltpu.make_async_remote_copy(src_ref=mine.at[turn], dst_ref=stats.at[turn, me], send_sem=stat_send.at[turn, k], recv_sem=stat_recv.at[turn, me], device_id=(device,), device_id_type=MESH))
            copies[-1].start()
        stats[turn, me] = row
        for k, device in enumerate(others):
            copies[k].wait_send()
            pltpu.make_async_remote_copy(src_ref=mine.at[turn], dst_ref=stats.at[turn, device], send_sem=stat_send.at[turn, k], recv_sem=stat_recv.at[turn, device], device_id=(device,), device_id_type=MESH).wait_recv()
        return jnp.sum(stats[turn], axis=0)

    def sum_square(values):
        return jnp.sum(values * values)

    grads = ((g1, g3), (g2, g4))
    scale = 1.0 / GROUP
    local = sum_square(g1[...] * scale) + sum_square(g3[...] * scale) + sum_square(g2[...] * scale) + sum_square(g4[...] * scale)
    total = share(0, jnp.full((8, 128), local, F32))
    norm = jnp.sqrt(total)
    clip = jnp.minimum(1.0, scalars[1] / (norm + NORM_EPS))
    norm_out[...] = norm
    clip = clip[0:1, 0:1]
    bias_one = 1.0 - BETA_ONE ** STEP
    bias_two = 1.0 - BETA_TWO ** STEP
    lane = lax.broadcasted_iota(jnp.int32, (8, 128), 1)
    row = jnp.zeros((8, 128), F32)
    families = ((master_up, avg_up, sq_up, dir_up), (master_down, avg_down, sq_down, dir_down))
    for f, (master, avg, sq, direction) in enumerate(families):
        for i in (f, 2 + f, 4 + f):
            fetches[i].wait()
        for k in range(2):
            g = grads[f][k][...] * scale
            avg_new = BETA_ONE * avg[k] + (1.0 - BETA_ONE) * clip * g
            sq_new = BETA_TWO * sq[k] + (1.0 - BETA_TWO) * (clip * clip) * (g * g)
            u = (avg_new / bias_one) / (jnp.sqrt(sq_new / bias_two) + ADAM_EPS)
            avg[k] = avg_new
            sq[k] = sq_new
            direction[k] = u
            row = row + jnp.where(lane == 2 * f + k, sum_square(master[k]), 0.0) + jnp.where(lane == 4 + 2 * f + k, sum_square(u), 0.0)
        stores[2 + f].start()
        stores[4 + f].start()
    totals = share(1, row)

    def out_view(chunk, picks, flipped=None):
        index = []
        for axis in range(3):
            if axis in picks:
                index.append(slice(None))
            elif axis == flipped:
                index.append(1 - coords[axis])
            else:
                index.append(coords[axis])
        family, k, (start, size) = chunk
        if family == 0:
            return w_up_out.at[(k, *index, core, slice(None), pl.ds(start, size))]
        return w_down_out.at[(k, *index, core, pl.ds(start, size), slice(None))]

    def neighbour(axis):
        stride = (8, 4, 2)[axis]
        return me + stride * (1 - 2 * coords[axis])

    def remote(n, kind, src, dst, device):
        return pltpu.make_async_remote_copy(src_ref=src, dst_ref=dst, send_sem=send_sem.at[n, kind], recv_sem=recv_sem.at[n, kind], device_id=(device,), device_id_type=MESH)

    chunks = []
    for f, parts in enumerate((COLUMN_PARTS, ROW_PARTS)):
        for k in range(2):
            chunks += [(f, k, part) for part in parts]
    order = [ORDERS[n % 3] for n in range(CHUNKS)]
    pending = []
    rounds = [[], [], []]
    locals_ = []
    for f, (master, direction, send) in enumerate(((master_up, dir_up, send_up), (master_down, dir_down, send_down))):
        for k in range(2):
            i = 2 * f + k
            ratio = jnp.sqrt(totals[0:1, i:i + 1]) / jnp.sqrt(totals[0:1, 4 + i:5 + i])
            new = master[k] - scalars[0] * ratio * direction[k]
            master[k] = new
            send[k] = new.astype(BF16)
            for part in range(3):
                n = 3 * i + part
                start, size = chunks[n][2]
                if f == 0:
                    src = send.at[k, :, pl.ds(start, size)]
                else:
                    src = send.at[k, pl.ds(start, size), :]
                dst = out_view(chunks[n], ())
                rounds[0].append(remote(n, 0, src, dst, neighbour(order[n][0])))
                rounds[0][-1].start()
                pending.append(remote(n, 3, src, dst, sibling))
                pending[-1].start()
                locals_.append(pltpu.make_async_copy(src, dst, own_sem.at[n]))
                locals_[-1].start()
        stores[f].start()
    for turn in range(3):
        for n in range(CHUNKS):
            first, second, third = order[n]
            if turn == 0:
                locals_[n].wait()
            rounds[turn][n].wait()
            gathered = order[n][:turn]
            view = out_view(chunks[n], gathered, order[n][turn])
            pending.append(remote(n, 4 + turn, view, view, sibling))
            pending[-1].start()
            if turn < 2:
                view = out_view(chunks[n], order[n][:turn + 1])
                rounds[turn + 1].append(remote(n, turn + 1, view, view, neighbour(order[n][turn + 1])))
                rounds[turn + 1][-1].start()
    for copy in pending + stores:
        copy.wait()


def tail(scalars, grads, states):
    vmem = pl.BlockSpec(memory_space=pltpu.VMEM)
    any_space = pl.BlockSpec(memory_space=pl.ANY)
    up, down = (2, UP_ROWS, FF), (2, DOWN_ROWS, D)
    shape = jax.ShapeDtypeStruct
    return pl.pallas_call(
        tail_kernel,
        in_specs=[pl.BlockSpec(memory_space=pltpu.SMEM)] + [vmem] * 4 + [any_space] * 6,
        out_specs=[any_space] * 8 + [vmem],
        out_shape=[
            shape((2, 2, 2, 2, 2, UP_ROWS, FF), BF16),
            shape((2, 2, 2, 2, 2, DOWN_ROWS, D), BF16),
            shape(up, F32), shape(down, F32), shape(up, F32), shape(down, F32), shape(up, F32), shape(down, F32),
            shape((8, 128), F32),
        ],
        scratch_shapes=[
            pltpu.VMEM(up, BF16), pltpu.VMEM(down, BF16), pltpu.VMEM(up, F32), pltpu.VMEM(down, F32),
            pltpu.VMEM((2, 8, 128), F32), pltpu.VMEM((2, GROUP, 8, 128), F32),
            pltpu.SemaphoreType.DMA((2, GROUP)), pltpu.SemaphoreType.DMA((2, GROUP)),
            pltpu.SemaphoreType.DMA((CHUNKS, 7)), pltpu.SemaphoreType.DMA((CHUNKS, 7)), pltpu.SemaphoreType.DMA((CHUNKS,)),
            *[pltpu.VMEM(dims, F32) for dims in (up, down) * 3], pltpu.SemaphoreType.DMA((6,)), pltpu.SemaphoreType.DMA((6,)),
        ],
        compiler_params=pltpu.CompilerParams(collective_id=3, has_side_effects=True, vmem_limit_bytes=67043328),
    )(scalars, *grads, *states)


def solution(mesh):
    batch_rows = P("data", None)
    state_rows = P(None, "data", None)
    replicated = P()

    def device_step(act_in, grad_out, w_up, w_down, master_up, master_down, exp_avg_up, exp_avg_down, exp_sq_up, exp_sq_down, learn_rate, clip_norm):
        z_one = jnp.dot(act_in, w_up[0], preferred_element_type=F32)
        act_one = gelu_parts(z_one)[0].astype(BF16)
        hidden = jnp.dot(act_one, w_down[0], preferred_element_type=F32).astype(BF16)
        z_three = jnp.dot(hidden, w_up[1], preferred_element_type=F32)
        act_three = gelu_parts(z_three)[0].astype(BF16)
        g_four = jnp.dot(act_three.T, grad_out, preferred_element_type=F32)
        shard_three, shard_four, d_hidden, d_hidden_t = second_block(z_three, grad_out, w_down, hidden.T, g_four, w_up)
        shard_one, shard_two = first_block(z_one, d_hidden, w_down, d_hidden_t, act_one, act_in)[:2]
        scalars = jnp.stack([learn_rate, clip_norm])
        outs = tail(scalars, (shard_one, shard_two, shard_three, shard_four), (master_up, master_down, exp_avg_up, exp_avg_down, exp_sq_up, exp_sq_down))
        new_w_up = outs[0].reshape(2, D, FF)
        new_w_down = outs[1].reshape(2, FF, D)
        return (new_w_up, new_w_down, *outs[2:8], outs[8][0, 0])

    return jax.shard_map(device_step, mesh=mesh, in_specs=(batch_rows, batch_rows, replicated, replicated, state_rows, state_rows, state_rows, state_rows, state_rows, state_rows, replicated, replicated), out_specs=(replicated, replicated, state_rows, state_rows, state_rows, state_rows, state_rows, state_rows, replicated), check_vma=False)
```

```python
import functools

import jax
import jax.numpy as jnp
from jax import lax
from jax.experimental import pallas as pl
from jax.experimental.pallas import tpu as pltpu
from jax.sharding import PartitionSpec as P

STEP = 10
BETA_ONE = 0.9
BETA_TWO = 0.95
ADAM_EPS = 1e-8
NORM_EPS = 1e-6
INV_SQRT_TWO = 0.7071067811865476
INV_SQRT_TWO_PI = 0.3989422804014327

GROUP = 16
TOKENS = 4096
D = 896
FF = 4864
TILE = 256
STEPS = FF // TILE
UP_ROWS = D // GROUP
DOWN_ROWS = FF // GROUP
DOWN_UNIT = DOWN_ROWS // STEPS
LAG = 2
DRAIN = 1 + 3 * LAG
SLOTS = LAG + 3
SUM_SLOTS = 3 * LAG
BLOCK = 512
MESH = pl.DeviceIdType.MESH
F32 = jnp.float32
BF16 = jnp.bfloat16


def gelu_parts(pre_act):
    normal_cdf = 0.5 * (1.0 + lax.erf(pre_act * INV_SQRT_TWO))
    normal_pdf = jnp.exp(-0.5 * pre_act * pre_act) * INV_SQRT_TWO_PI
    return pre_act * normal_cdf, normal_cdf + pre_act * normal_pdf


def dot_last(left, right):
    return lax.dot_general(left, right, (((1,), (1,)), ((), ())), preferred_element_type=F32)


def greet(devices):
    barrier = pltpu.get_barrier_semaphore()
    for device in devices:
        pl.semaphore_signal(barrier, inc=1, device_id=(device,), device_id_type=MESH)
    pl.semaphore_wait(barrier, len(devices))


class ReduceScatter:
    def __init__(self, phase, gbuf, rc, sums, r1, r2, r3, send, recv):
        self.phase = phase
        self.gbuf, self.rc, self.sums, self.landed = gbuf, rc, sums, (r1, r2, r3)
        self.send, self.recv = send, recv
        self.me = lax.axis_index("data")
        self.core = lax.rem(self.me, 2)
        self.chip = self.me // 2

    def stride_bit(self, unit, stage):
        axis = lax.rem(unit + self.phase + (0, 2, 1)[stage - 1], 3)
        stride = 1 + axis + axis * (axis - 1) // 2
        return stride, lax.rem(self.chip // stride, 2)

    def copy(self, stage, unit):
        if stage == 0:
            slot = lax.rem(unit, 2)
            src, dst = self.gbuf.at[slot, :, 1 - self.core], self.rc.at[slot]
            device = self.me + 1 - 2 * self.core
        else:
            slot = lax.rem(unit, SLOTS)
            count = 8 >> stage
            src = self.sums.at[lax.rem(unit, SUM_SLOTS), pl.ds(count, count)]
            dst = self.landed[stage - 1].at[slot]
            stride, bit = self.stride_bit(unit, stage)
            device = self.me + 2 * stride * (1 - 2 * bit)
        return pltpu.make_async_remote_copy(src_ref=src, dst_ref=dst, send_sem=self.send.at[stage, slot], recv_sem=self.recv.at[stage, slot], device_id=(device,), device_id_type=MESH)

    def finish(self, stage, unit):
        self.copy(stage, unit).wait()
        held = lax.rem(unit, SUM_SLOTS)
        if stage == 0:
            slot = lax.rem(unit, 2)
            parts = [self.stride_bit(unit, s) for s in (1, 2, 3)]
            for pos in range(8):
                chip = 0
                for (stride, bit), flip in zip(parts, (pos // 4, pos // 2 % 2, pos % 2)):
                    chip = chip + (1 - bit if flip else bit) * stride
                self.sums[held, pos] = self.gbuf[slot, chip, self.core] + self.rc[slot, chip]
        elif stage < 3:
            count = 8 >> stage
            slot = lax.rem(unit, SLOTS)
            for pos in range(count):
                self.sums[held, pos] = self.sums[held, pos] + self.landed[stage - 1][slot, pos]
        else:
            return self.sums[held, 0] + self.landed[2][lax.rem(unit, SLOTS), 0]


FLUSHES = TOKENS // BLOCK
assert FLUSHES <= DRAIN + 1


def within(unit, count):
    return jnp.logical_and(unit >= 0, unit < count)


def advance(ring, tick, count, emit):
    @pl.when(within(tick - DRAIN, count))
    def _():
        emit(tick - DRAIN, ring.finish(3, tick - DRAIN))

    for stage in (2, 1, 0):
        unit = tick - 1 - stage * LAG

        @pl.when(within(unit, count))
        def _():
            ring.finish(stage, unit)
            ring.copy(stage + 1, unit).start()


def greet_partners(ring):
    me, core, chip = ring.me, ring.core, ring.chip
    greet([me + 1 - 2 * core] + [me + 2 * s * (1 - 2 * lax.rem(chip // s, 2)) for s in (1, 2, 4)])


def aligned(index, size):
    return pl.ds(pl.multiple_of(index * size, size), size)


def grad_tile(z_ref, dy_ref, wd_ref, qbuf, size, extra):
    def block(index, carry):
        rows = aligned(index, size)
        slope = gelu_parts(z_ref[rows, :])[1]
        grad = (dot_last(dy_ref[rows, :], wd_ref[...]) * slope).astype(BF16)
        qbuf[rows, :] = grad
        extra(rows, grad)
        return carry

    lax.fori_loop(0, TOKENS // size, block, 0, unroll=TOKENS // size)


def store_tile(left, qbuf, gbuf, slot):
    tile = jnp.dot(left[...], qbuf[...], preferred_element_type=F32)
    for i in range(GROUP):
        gbuf[slot, i // 2, i % 2] = tile[i * UP_ROWS:(i + 1) * UP_ROWS, :]


def second_block_kernel(z_ref, dy_ref, wd_ref, left_ref, gd_ref, wu_ref, up_ref, down_ref, dx_ref, dxt_ref, qbuf, acc, stage_buf, stage_t, *rest):
    up = ReduceScatter(0, *rest[0:8])
    down = ReduceScatter(1, *rest[8:16])
    load_sem, out_sem = rest[16:18]
    step = pl.program_id(0)

    def load(unit):
        slot = lax.rem(unit, 2)
        return pltpu.make_async_copy(gd_ref.at[:, :, aligned(unit, DOWN_UNIT)], down.gbuf.at[slot], load_sem.at[slot])

    @pl.when(step == 0)
    def _():
        greet_partners(up)
        load(0).start()
        acc[...] = jnp.zeros_like(acc)

    def add_dx(rows, grad):
        acc[rows, :] += dot_last(grad, wu_ref[...])

    @pl.when(step < STEPS)
    def _():
        grad_tile(z_ref, dy_ref, wd_ref, qbuf, BLOCK // 2, add_dx)
        store_tile(left_ref, qbuf, up.gbuf, lax.rem(step, 2))

    def emit_up(unit, block):
        up_ref[:, aligned(unit, TILE)] = block

    def emit_down(unit, block):
        down_ref[aligned(unit, DOWN_UNIT), :] = block

    advance(up, step, STEPS, emit_up)
    advance(down, step, STEPS, emit_down)

    @pl.when(step < STEPS - 1)
    def _():
        load(step + 1).start()

    @pl.when(step < STEPS)
    def _():
        up.copy(0, step).start()
        load(step).wait()
        down.copy(0, step).start()

    turn = step - (STEPS - 1)

    def outs(index):
        rows = aligned(index, BLOCK)
        return [pltpu.make_async_copy(stage_buf, dx_ref.at[rows, :], out_sem.at[0]), pltpu.make_async_copy(stage_t, dxt_ref.at[:, rows], out_sem.at[1])]

    @pl.when(jnp.logical_and(turn >= 1, turn < FLUSHES))
    def _():
        for copy in outs(turn - 1):
            copy.wait()

    @pl.when(within(turn, FLUSHES))
    def _():
        value = acc[aligned(turn, BLOCK), :]
        stage_buf[...] = value.astype(BF16)
        stage_t[...] = value.T.astype(BF16)
        for copy in outs(turn):
            copy.start()

    @pl.when(turn == FLUSHES - 1)
    def _():
        for copy in outs(turn):
            copy.wait()


def first_block_kernel(z_ref, dy_ref, wd_ref, dyt_ref, act_ref, x_ref, up_ref, down_ref, gd_ref, qbuf, left, stage_buf, act_buf, act_sem, *rest):
    up = ReduceScatter(0, *rest[0:8])
    down = ReduceScatter(1, *rest[8:16])
    load_sem, out_sem = rest[16:18]
    step = pl.program_id(0)

    def loads(unit):
        slot = lax.rem(unit, 2)
        columns, half = aligned(unit // 2, LANES), lax.rem(unit, 2) * HALF_ROWS
        copies = []
        for i in range(GROUP):
            rows = pl.ds(pl.multiple_of(i * DOWN_ROWS + half, 8), HALF_ROWS)
            copies.append(pltpu.make_async_copy(gd_ref.at[rows, columns], down.gbuf.at[slot, i // 2, i % 2], load_sem.at[slot, i]))
        return copies

    def write(index, split):
        slot = lax.rem(index, 2)
        rows = aligned(lax.rem(index, STEPS), TILE)
        if split == 0:
            return pltpu.make_async_copy(stage_buf.at[slot, :, pl.ds(0, SPLIT)], gd_ref.at[rows, pl.ds(0, SPLIT)], out_sem.at[slot])
        return pltpu.make_async_copy(stage_buf.at[slot, :, pl.ds(0, D - SPLIT)], gd_ref.at[rows, pl.ds(SPLIT, D - SPLIT)], out_sem.at[slot])

    def fetch(index):
        slot = lax.rem(index, ACT_SLOTS)
        return pltpu.make_async_copy(act_ref.at[:, aligned(lax.rem(index, STEPS), TILE)], act_buf.at[slot], act_sem.at[slot])

    @pl.when(step == 0)
    def _():
        for index in range(ACT_SLOTS):
            fetch(index).start()
        greet_partners(up)

    @pl.when(step < TOKENS // TILE)
    def _():
        left[:, aligned(step, TILE)] = x_ref[...].T

    @pl.when(step < 2 * STEPS)
    def _():
        fetch(step).wait()

    for split in (0, 1):
        @pl.when(within(step - split * STEPS, STEPS))
        def _():
            width = SPLIT if split == 0 else D - SPLIT
            part = jnp.dot(dyt_ref[pl.ds(split * SPLIT, width), :], act_buf[lax.rem(step, ACT_SLOTS)], preferred_element_type=F32)
            stage_buf[lax.rem(step, 2), :, pl.ds(0, width)] = part.T

    @pl.when(step < 2 * STEPS - ACT_SLOTS)
    def _():
        fetch(step + ACT_SLOTS).start()

    for split in (0, 1):
        @pl.when(within(step - 1 - split * STEPS, STEPS))
        def _():
            write(step - 1, split).wait()

    for split in (0, 1):
        @pl.when(within(step - split * STEPS, STEPS))
        def _():
            write(step, split).start()

    tile = step - 2 * STEPS

    @pl.when(within(tile, STEPS))
    def _():
        grad_tile(z_ref, dy_ref, wd_ref, qbuf, BLOCK, lambda rows, grad: None)
        store_tile(left, qbuf, up.gbuf, lax.rem(tile, 2))

    def emit_up(unit, block):
        up_ref[:, aligned(unit, TILE)] = block

    def emit_down(unit, block):
        down_ref[pl.ds(pl.multiple_of(lax.rem(unit, 2) * HALF_ROWS, 8), HALF_ROWS), aligned(unit // 2, LANES)] = block

    early = step - FIRST_TICK
    ticking = jnp.logical_or(jnp.logical_and(early >= 0, lax.rem(early, TICK_GAP) == 0), tile >= 0)
    tick = jnp.where(tile >= 0, tile + (2 * STEPS - FIRST_TICK) // TICK_GAP, early // TICK_GAP)
    tick = jnp.where(ticking, tick, -1)

    advance(up, tile, STEPS, emit_up)
    advance(down, tick, DOWN_UNITS, emit_down)

    @pl.when(step == FIRST_TICK - 1)
    def _():
        for copy in loads(0):
            copy.start()

    @pl.when(within(tick, DOWN_UNITS - 1))
    def _():
        for copy in loads(tick + 1):
            copy.start()

    @pl.when(within(tile, STEPS))
    def _():
        up.copy(0, tile).start()

    @pl.when(within(tick, DOWN_UNITS))
    def _():
        for copy in loads(tick):
            copy.wait()
        down.copy(0, tick).start()


def ring_scratch(rows, columns):
    block = (rows, columns)
    return [
        pltpu.VMEM((2, 8, 2) + block, F32),
        pltpu.VMEM((2, 8) + block, F32),
        pltpu.VMEM((SUM_SLOTS, 8) + block, F32),
        pltpu.VMEM((SLOTS, 4) + block, F32),
        pltpu.VMEM((SLOTS, 2) + block, F32),
        pltpu.VMEM((SLOTS, 1) + block, F32),
        pltpu.SemaphoreType.DMA((4, SLOTS)),
        pltpu.SemaphoreType.DMA((4, SLOTS)),
    ]


WHOLE = pl.Buffered(buffer_count=1)
ANY = pl.BlockSpec(memory_space=pl.ANY)


def params(collective_id):
    return pltpu.CompilerParams(collective_id=collective_id, has_side_effects=True, vmem_limit_bytes=67043328, dimension_semantics=("arbitrary",))


def second_block(pre_act, grad, w_down, left, grad_down, w_up):
    last = STEPS - 1
    return pl.pallas_call(
        second_block_kernel,
        grid=(STEPS + DRAIN,),
        in_specs=[
            pl.BlockSpec((TOKENS, TILE), lambda s: (0, jnp.minimum(s, last))),
            pl.BlockSpec((TOKENS, D), lambda s: (0, 0), pipeline_mode=WHOLE),
            pl.BlockSpec((None, TILE, D), lambda s: (1, jnp.minimum(s, last), 0)),
            pl.BlockSpec((D, TOKENS), lambda s: (0, 0), pipeline_mode=WHOLE),
            ANY,
            pl.BlockSpec((None, D, TILE), lambda s: (1, 0, jnp.minimum(s, last))),
        ],
        out_specs=[pl.BlockSpec((UP_ROWS, FF), lambda s: (0, 0)), pl.BlockSpec((DOWN_ROWS, D), lambda s: (0, 0)), ANY, ANY],
        out_shape=[jax.ShapeDtypeStruct((UP_ROWS, FF), F32), jax.ShapeDtypeStruct((DOWN_ROWS, D), F32), jax.ShapeDtypeStruct((TOKENS, D), BF16), jax.ShapeDtypeStruct((D, TOKENS), BF16)],
        scratch_shapes=[pltpu.VMEM((TOKENS, TILE), BF16), pltpu.VMEM((TOKENS, D), F32), pltpu.VMEM((BLOCK, D), BF16), pltpu.VMEM((D, BLOCK), BF16)] + ring_scratch(UP_ROWS, TILE) + ring_scratch(DOWN_UNIT, D) + [pltpu.SemaphoreType.DMA((2,)), pltpu.SemaphoreType.DMA((2,))],
        compiler_params=params(1),
        cost_estimate=pl.CostEstimate(flops=6 * TOKENS * D * FF, bytes_accessed=150 * 2**20, transcendentals=2 * TOKENS * FF),
    )(pre_act, grad, w_down, left, grad_down.reshape(8, 2, DOWN_ROWS, D), w_up)


LANES = 128
HALF_ROWS = DOWN_ROWS // 2
DOWN_UNITS = 2 * D // LANES
SPLIT = 512
TICK_GAP = 4
ACT_SLOTS = 3
FIRST_TICK = STEPS + 3


def first_block(pre_act, grad, w_down, grad_t, act, act_in):
    start, last = 2 * STEPS, STEPS - 1
    return pl.pallas_call(
        first_block_kernel,
        grid=(start + STEPS + DRAIN,),
        in_specs=[
            pl.BlockSpec((TOKENS, TILE), lambda s: (0, jnp.clip(s - start, 0, last))),
            pl.BlockSpec((TOKENS, D), lambda s: (0, 0), pipeline_mode=WHOLE),
            pl.BlockSpec((None, TILE, D), lambda s: (0, jnp.clip(s - start, 0, last), 0)),
            pl.BlockSpec((D, TOKENS), lambda s: (0, 0), pipeline_mode=WHOLE),
            ANY,
            pl.BlockSpec((TILE, D), lambda s: (jnp.minimum(s, TOKENS // TILE - 1), 0)),
        ],
        out_specs=[pl.BlockSpec((UP_ROWS, FF), lambda s: (0, 0)), pl.BlockSpec((DOWN_ROWS, D), lambda s: (0, 0)), ANY],
        out_shape=[jax.ShapeDtypeStruct((UP_ROWS, FF), F32), jax.ShapeDtypeStruct((DOWN_ROWS, D), F32), jax.ShapeDtypeStruct((FF, D), F32)],
        scratch_shapes=[pltpu.VMEM((TOKENS, TILE), BF16), pltpu.VMEM((D, TOKENS), BF16), pltpu.VMEM((2, TILE, SPLIT), F32), pltpu.VMEM((ACT_SLOTS, TOKENS, TILE), BF16), pltpu.SemaphoreType.DMA((ACT_SLOTS,))] + ring_scratch(UP_ROWS, TILE) + ring_scratch(HALF_ROWS, LANES) + [pltpu.SemaphoreType.DMA((2, GROUP)), pltpu.SemaphoreType.DMA((2,))],
        compiler_params=params(2),
        cost_estimate=pl.CostEstimate(flops=6 * TOKENS * D * FF, bytes_accessed=250 * 2**20, transcendentals=2 * TOKENS * FF),
    )(pre_act, grad, w_down, grad_t, act, act_in)


COLUMN_PARTS = ((0, 1664), (1664, 1664), (3328, 1536))
ROW_PARTS = ((0, 112), (112, 96), (208, 96))
ORDERS = ((2, 1, 0), (1, 0, 2), (0, 2, 1))
CHUNKS = 12


def tail_kernel(scalars, g1, g2, g3, g4, *refs):
    states, (w_up_out, w_down_out), state_outs, norm_out = refs[:6], refs[6:8], refs[8:14], refs[14]
    send_up, send_down, dir_up, dir_down, mine, stats, stat_send, stat_recv, send_sem, recv_sem, own_sem = refs[15:26]
    held, (in_sem, out_sem) = refs[26:32], refs[32:34]
    master_up, master_down, avg_up, avg_down, sq_up, sq_down = held
    fetches = [pltpu.make_async_copy(src, dst, in_sem.at[i]) for i, (src, dst) in enumerate(zip(states, held))]
    stores = [pltpu.make_async_copy(src, dst, out_sem.at[i]) for i, (src, dst) in enumerate(zip(held, state_outs))]
    for copy in fetches:
        copy.start()
    me = lax.axis_index("data")
    core = lax.rem(me, 2)
    coords = (me // 8, lax.rem(me // 4, 2), lax.rem(me // 2, 2))
    sibling = me + 1 - 2 * core
    others = [lax.rem(me + k, GROUP) for k in range(1, GROUP)]
    greet(others)

    def share(turn, row):
        mine[turn] = row
        copies = []
        for k, device in enumerate(others):
            copies.append(pltpu.make_async_remote_copy(src_ref=mine.at[turn], dst_ref=stats.at[turn, me], send_sem=stat_send.at[turn, k], recv_sem=stat_recv.at[turn, me], device_id=(device,), device_id_type=MESH))
            copies[-1].start()
        stats[turn, me] = row
        for k, device in enumerate(others):
            copies[k].wait_send()
            pltpu.make_async_remote_copy(src_ref=mine.at[turn], dst_ref=stats.at[turn, device], send_sem=stat_send.at[turn, k], recv_sem=stat_recv.at[turn, device], device_id=(device,), device_id_type=MESH).wait_recv()
        return jnp.sum(stats[turn], axis=0)

    def sum_square(values):
        return jnp.sum(values * values)

    grads = ((g1, g3), (g2, g4))
    scale = 1.0 / GROUP
    local = sum_square(g1[...] * scale) + sum_square(g3[...] * scale) + sum_square(g2[...] * scale) + sum_square(g4[...] * scale)
    total = share(0, jnp.full((8, 128), local, F32))
    norm = jnp.sqrt(total)
    clip = jnp.minimum(1.0, scalars[1] / (norm + NORM_EPS))
    norm_out[...] = norm
    clip = clip[0:1, 0:1]
    bias_one = 1.0 - BETA_ONE ** STEP
    bias_two = 1.0 - BETA_TWO ** STEP
    lane = lax.broadcasted_iota(jnp.int32, (8, 128), 1)
    row = jnp.zeros((8, 128), F32)
    families = ((master_up, avg_up, sq_up, dir_up), (master_down, avg_down, sq_down, dir_down))
    for f, (master, avg, sq, direction) in enumerate(families):
        for i in (f, 2 + f, 4 + f):
            fetches[i].wait()
        for k in range(2):
            g = grads[f][k][...] * scale
            avg_new = BETA_ONE * avg[k] + (1.0 - BETA_ONE) * clip * g
            sq_new = BETA_TWO * sq[k] + (1.0 - BETA_TWO) * (clip * clip) * (g * g)
            u = (avg_new / bias_one) / (jnp.sqrt(sq_new / bias_two) + ADAM_EPS)
            avg[k] = avg_new
            sq[k] = sq_new
            direction[k] = u
            row = row + jnp.where(lane == 2 * f + k, sum_square(master[k]), 0.0) + jnp.where(lane == 4 + 2 * f + k, sum_square(u), 0.0)
        stores[2 + f].start()
        stores[4 + f].start()
    totals = share(1, row)

    def out_view(chunk, picks, flipped=None):
        index = []
        for axis in range(3):
            if axis in picks:
                index.append(slice(None))
            elif axis == flipped:
                index.append(1 - coords[axis])
            else:
                index.append(coords[axis])
        family, k, (start, size) = chunk
        if family == 0:
            return w_up_out.at[(k, *index, core, slice(None), pl.ds(start, size))]
        return w_down_out.at[(k, *index, core, pl.ds(start, size), slice(None))]

    def neighbour(axis):
        stride = (8, 4, 2)[axis]
        return me + stride * (1 - 2 * coords[axis])

    def remote(n, kind, src, dst, device):
        return pltpu.make_async_remote_copy(src_ref=src, dst_ref=dst, send_sem=send_sem.at[n, kind], recv_sem=recv_sem.at[n, kind], device_id=(device,), device_id_type=MESH)

    chunks = []
    for f, parts in enumerate((COLUMN_PARTS, ROW_PARTS)):
        for k in range(2):
            chunks += [(f, k, part) for part in parts]
    order = [ORDERS[n % 3] for n in range(CHUNKS)]
    pending = []
    rounds = [[], [], []]
    locals_ = []
    for f, (master, direction, send) in enumerate(((master_up, dir_up, send_up), (master_down, dir_down, send_down))):
        for k in range(2):
            i = 2 * f + k
            ratio = jnp.sqrt(totals[0:1, i:i + 1]) / jnp.sqrt(totals[0:1, 4 + i:5 + i])
            new = master[k] - scalars[0] * ratio * direction[k]
            master[k] = new
            send[k] = new.astype(BF16)
            for part in range(3):
                n = 3 * i + part
                start, size = chunks[n][2]
                if f == 0:
                    src = send.at[k, :, pl.ds(start, size)]
                else:
                    src = send.at[k, pl.ds(start, size), :]
                dst = out_view(chunks[n], ())
                rounds[0].append(remote(n, 0, src, dst, neighbour(order[n][0])))
                rounds[0][-1].start()
                pending.append(remote(n, 3, src, dst, sibling))
                pending[-1].start()
                locals_.append(pltpu.make_async_copy(src, dst, own_sem.at[n]))
                locals_[-1].start()
        stores[f].start()
    for turn in range(3):
        for n in range(CHUNKS):
            first, second, third = order[n]
            if turn == 0:
                locals_[n].wait()
            rounds[turn][n].wait()
            gathered = order[n][:turn]
            view = out_view(chunks[n], gathered, order[n][turn])
            pending.append(remote(n, 4 + turn, view, view, sibling))
            pending[-1].start()
            if turn < 2:
                view = out_view(chunks[n], order[n][:turn + 1])
                rounds[turn + 1].append(remote(n, turn + 1, view, view, neighbour(order[n][turn + 1])))
                rounds[turn + 1][-1].start()
    for copy in pending + stores:
        copy.wait()


def tail(scalars, grads, states):
    vmem = pl.BlockSpec(memory_space=pltpu.VMEM)
    any_space = pl.BlockSpec(memory_space=pl.ANY)
    up, down = (2, UP_ROWS, FF), (2, DOWN_ROWS, D)
    shape = jax.ShapeDtypeStruct
    return pl.pallas_call(
        tail_kernel,
        in_specs=[pl.BlockSpec(memory_space=pltpu.SMEM)] + [vmem] * 4 + [any_space] * 6,
        out_specs=[any_space] * 8 + [vmem],
        out_shape=[
            shape((2, 2, 2, 2, 2, UP_ROWS, FF), BF16),
            shape((2, 2, 2, 2, 2, DOWN_ROWS, D), BF16),
            shape(up, F32), shape(down, F32), shape(up, F32), shape(down, F32), shape(up, F32), shape(down, F32),
            shape((8, 128), F32),
        ],
        scratch_shapes=[
            pltpu.VMEM(up, BF16), pltpu.VMEM(down, BF16), pltpu.VMEM(up, F32), pltpu.VMEM(down, F32),
            pltpu.VMEM((2, 8, 128), F32), pltpu.VMEM((2, GROUP, 8, 128), F32),
            pltpu.SemaphoreType.DMA((2, GROUP)), pltpu.SemaphoreType.DMA((2, GROUP)),
            pltpu.SemaphoreType.DMA((CHUNKS, 7)), pltpu.SemaphoreType.DMA((CHUNKS, 7)), pltpu.SemaphoreType.DMA((CHUNKS,)),
            *[pltpu.VMEM(dims, F32) for dims in (up, down) * 3], pltpu.SemaphoreType.DMA((6,)), pltpu.SemaphoreType.DMA((6,)),
        ],
        compiler_params=pltpu.CompilerParams(collective_id=3, has_side_effects=True, vmem_limit_bytes=67043328),
    )(scalars, *grads, *states)


def solution(mesh):
    batch_rows = P("data", None)
    state_rows = P(None, "data", None)
    replicated = P()

    def device_step(act_in, grad_out, w_up, w_down, master_up, master_down, exp_avg_up, exp_avg_down, exp_sq_up, exp_sq_down, learn_rate, clip_norm):
        z_one = jnp.dot(act_in, w_up[0], preferred_element_type=F32)
        act_one = gelu_parts(z_one)[0].astype(BF16)
        hidden = jnp.dot(act_one, w_down[0], preferred_element_type=F32).astype(BF16)
        z_three = jnp.dot(hidden, w_up[1], preferred_element_type=F32)
        act_three = gelu_parts(z_three)[0].astype(BF16)
        g_four = jnp.dot(act_three.T, grad_out, preferred_element_type=F32)
        shard_three, shard_four, d_hidden, d_hidden_t = second_block(z_three, grad_out, w_down, hidden.T, g_four, w_up)
        shard_one, shard_two = first_block(z_one, d_hidden, w_down, d_hidden_t, act_one, act_in)[:2]
        scalars = jnp.stack([learn_rate, clip_norm])
        outs = tail(scalars, (shard_one, shard_two, shard_three, shard_four), (master_up, master_down, exp_avg_up, exp_avg_down, exp_sq_up, exp_sq_down))
        new_w_up = outs[0].reshape(2, D, FF)
        new_w_down = outs[1].reshape(2, FF, D)
        return (new_w_up, new_w_down, *outs[2:8], outs[8][0, 0])

    return jax.shard_map(device_step, mesh=mesh, in_specs=(batch_rows, batch_rows, replicated, replicated, state_rows, state_rows, state_rows, state_rows, state_rows, state_rows, replicated, replicated), out_specs=(replicated, replicated, state_rows, state_rows, state_rows, state_rows, state_rows, state_rows, replicated), check_vma=False)
```

```python
import functools

import jax
import jax.numpy as jnp
from jax import lax
from jax.experimental import pallas as pl
from jax.experimental.pallas import tpu as pltpu
from jax.sharding import PartitionSpec as P

STEP = 10
BETA_ONE = 0.9
BETA_TWO = 0.95
ADAM_EPS = 1e-8
NORM_EPS = 1e-6
INV_SQRT_TWO = 0.7071067811865476
INV_SQRT_TWO_PI = 0.3989422804014327

GROUP = 16
TOKENS = 4096
D = 896
FF = 4864
TILE = 256
STEPS = FF // TILE
UP_ROWS = D // GROUP
DOWN_ROWS = FF // GROUP
DOWN_UNIT = DOWN_ROWS // STEPS
LAG = 2
DRAIN = 1 + 3 * LAG
SLOTS = LAG + 3
SUM_SLOTS = 3 * LAG
BLOCK = 512
MESH = pl.DeviceIdType.MESH
F32 = jnp.float32
BF16 = jnp.bfloat16


def gelu_parts(pre_act):
    normal_cdf = 0.5 * (1.0 + lax.erf(pre_act * INV_SQRT_TWO))
    normal_pdf = jnp.exp(-0.5 * pre_act * pre_act) * INV_SQRT_TWO_PI
    return pre_act * normal_cdf, normal_cdf + pre_act * normal_pdf


def dot_last(left, right):
    return lax.dot_general(left, right, (((1,), (1,)), ((), ())), preferred_element_type=F32)


def greet(devices):
    barrier = pltpu.get_barrier_semaphore()
    for device in devices:
        pl.semaphore_signal(barrier, inc=1, device_id=(device,), device_id_type=MESH)
    pl.semaphore_wait(barrier, len(devices))


class ReduceScatter:
    def __init__(self, phase, gbuf, rc, sums, r1, r2, r3, send, recv):
        self.phase = phase
        self.gbuf, self.rc, self.sums, self.landed = gbuf, rc, sums, (r1, r2, r3)
        self.send, self.recv = send, recv
        self.me = lax.axis_index("data")
        self.core = lax.rem(self.me, 2)
        self.chip = self.me // 2

    def stride_bit(self, unit, stage):
        axis = lax.rem(unit + self.phase + (0, 2, 1)[stage - 1], 3)
        stride = 1 + axis + axis * (axis - 1) // 2
        return stride, lax.rem(self.chip // stride, 2)

    def copy(self, stage, unit):
        if stage == 0:
            slot = lax.rem(unit, 2)
            src, dst = self.gbuf.at[slot, :, 1 - self.core], self.rc.at[slot]
            device = self.me + 1 - 2 * self.core
        else:
            slot = lax.rem(unit, SLOTS)
            count = 8 >> stage
            src = self.sums.at[lax.rem(unit, SUM_SLOTS), pl.ds(count, count)]
            dst = self.landed[stage - 1].at[slot]
            stride, bit = self.stride_bit(unit, stage)
            device = self.me + 2 * stride * (1 - 2 * bit)
        return pltpu.make_async_remote_copy(src_ref=src, dst_ref=dst, send_sem=self.send.at[stage, slot], recv_sem=self.recv.at[stage, slot], device_id=(device,), device_id_type=MESH)

    def finish(self, stage, unit):
        self.copy(stage, unit).wait()
        held = lax.rem(unit, SUM_SLOTS)
        if stage == 0:
            slot = lax.rem(unit, 2)
            parts = [self.stride_bit(unit, s) for s in (1, 2, 3)]
            for pos in range(8):
                chip = 0
                for (stride, bit), flip in zip(parts, (pos // 4, pos // 2 % 2, pos % 2)):
                    chip = chip + (1 - bit if flip else bit) * stride
                self.sums[held, pos] = self.gbuf[slot, chip, self.core] + self.rc[slot, chip]
        elif stage < 3:
            count = 8 >> stage
            slot = lax.rem(unit, SLOTS)
            for pos in range(count):
                self.sums[held, pos] = self.sums[held, pos] + self.landed[stage - 1][slot, pos]
        else:
            return self.sums[held, 0] + self.landed[2][lax.rem(unit, SLOTS), 0]


FLUSHES = TOKENS // BLOCK
assert FLUSHES <= DRAIN + 1


def within(unit, count):
    return jnp.logical_and(unit >= 0, unit < count)


def advance(ring, tick, count, emit):
    @pl.when(within(tick - DRAIN, count))
    def _():
        emit(tick - DRAIN, ring.finish(3, tick - DRAIN))

    for stage in (2, 1, 0):
        unit = tick - 1 - stage * LAG

        @pl.when(within(unit, count))
        def _():
            ring.finish(stage, unit)
            ring.copy(stage + 1, unit).start()


def greet_partners(ring):
    me, core, chip = ring.me, ring.core, ring.chip
    greet([me + 1 - 2 * core] + [me + 2 * s * (1 - 2 * lax.rem(chip // s, 2)) for s in (1, 2, 4)])


def aligned(index, size):
    return pl.ds(pl.multiple_of(index * size, size), size)


def grad_tile(z_ref, dy_ref, wd_ref, qbuf, size, extra):
    def block(index, carry):
        rows = aligned(index, size)
        slope = gelu_parts(z_ref[rows, :])[1]
        grad = (dot_last(dy_ref[rows, :], wd_ref[...]) * slope).astype(BF16)
        qbuf[rows, :] = grad
        extra(rows, grad)
        return carry

    lax.fori_loop(0, TOKENS // size, block, 0, unroll=TOKENS // size)


def store_tile(left, qbuf, gbuf, slot):
    tile = jnp.dot(left[...], qbuf[...], preferred_element_type=F32)
    for i in range(GROUP):
        gbuf[slot, i // 2, i % 2] = tile[i * UP_ROWS:(i + 1) * UP_ROWS, :]


def second_block_kernel(z_ref, dy_ref, wd_ref, left_ref, gd_ref, wu_ref, up_ref, down_ref, dx_ref, dxt_ref, qbuf, acc, stage_buf, stage_t, *rest):
    up = ReduceScatter(0, *rest[0:8])
    down = ReduceScatter(1, *rest[8:16])
    load_sem, out_sem = rest[16:18]
    step = pl.program_id(0)

    def load(unit):
        slot = lax.rem(unit, 2)
        return pltpu.make_async_copy(gd_ref.at[:, :, aligned(unit, DOWN_UNIT)], down.gbuf.at[slot], load_sem.at[slot])

    @pl.when(step == 0)
    def _():
        greet_partners(up)
        load(0).start()
        acc[...] = jnp.zeros_like(acc)

    def add_dx(rows, grad):
        acc[rows, :] += dot_last(grad, wu_ref[...])

    @pl.when(step < STEPS)
    def _():
        grad_tile(z_ref, dy_ref, wd_ref, qbuf, BLOCK // 2, add_dx)
        store_tile(left_ref, qbuf, up.gbuf, lax.rem(step, 2))

    def emit_up(unit, block):
        up_ref[:, aligned(unit, TILE)] = block

    def emit_down(unit, block):
        down_ref[aligned(unit, DOWN_UNIT), :] = block

    advance(up, step, STEPS, emit_up)
    advance(down, step, STEPS, emit_down)

    @pl.when(step < STEPS - 1)
    def _():
        load(step + 1).start()

    @pl.when(step < STEPS)
    def _():
        up.copy(0, step).start()
        load(step).wait()
        down.copy(0, step).start()

    turn = step - (STEPS - 1)

    def outs(index):
        rows = aligned(index, BLOCK)
        return [pltpu.make_async_copy(stage_buf, dx_ref.at[rows, :], out_sem.at[0]), pltpu.make_async_copy(stage_t, dxt_ref.at[:, rows], out_sem.at[1])]

    @pl.when(jnp.logical_and(turn >= 1, turn < FLUSHES))
    def _():
        for copy in outs(turn - 1):
            copy.wait()

    @pl.when(within(turn, FLUSHES))
    def _():
        value = acc[aligned(turn, BLOCK), :]
        stage_buf[...] = value.astype(BF16)
        stage_t[...] = value.T.astype(BF16)
        for copy in outs(turn):
            copy.start()

    @pl.when(turn == FLUSHES - 1)
    def _():
        for copy in outs(turn):
            copy.wait()


def first_block_kernel(z_ref, dy_ref, wd_ref, dyt_ref, act_ref, x_ref, up_ref, down_ref, gd_ref, qbuf, left, stage_buf, act_buf, act_sem, *rest):
    up = ReduceScatter(0, *rest[0:8])
    down = ReduceScatter(1, *rest[8:16])
    load_sem, out_sem = rest[16:18]
    step = pl.program_id(0)

    def loads(unit):
        slot = lax.rem(unit, 2)
        columns, half = aligned(unit // 2, LANES), lax.rem(unit, 2) * HALF_ROWS
        copies = []
        for i in range(GROUP):
            rows = pl.ds(pl.multiple_of(i * DOWN_ROWS + half, 8), HALF_ROWS)
            copies.append(pltpu.make_async_copy(gd_ref.at[rows, columns], down.gbuf.at[slot, i // 2, i % 2], load_sem.at[slot, i]))
        return copies

    def write(index):
        slot = lax.rem(index, 2)
        return pltpu.make_async_copy(stage_buf.at[slot], gd_ref.at[aligned(index, TILE), :], out_sem.at[slot])

    def fetch(index):
        slot = lax.rem(index, ACT_SLOTS)
        return pltpu.make_async_copy(act_ref.at[:, aligned(index, TILE)], act_buf.at[slot], act_sem.at[slot])

    @pl.when(step == 0)
    def _():
        for index in range(ACT_SLOTS):
            fetch(index).start()
        greet_partners(up)

    @pl.when(step < TOKENS // TILE)
    def _():
        left[:, aligned(step, TILE)] = x_ref[...].T

    @pl.when(step < STEPS)
    def _():
        fetch(step).wait()
        part = jnp.dot(dyt_ref[...], act_buf[lax.rem(step, ACT_SLOTS)], preferred_element_type=F32)
        stage_buf[lax.rem(step, 2)] = part.T

    @pl.when(step < STEPS - ACT_SLOTS)
    def _():
        fetch(step + ACT_SLOTS).start()

    @pl.when(within(step - 1, STEPS))
    def _():
        write(step - 1).wait()

    @pl.when(step < STEPS)
    def _():
        write(step).start()

    tile = step - STEPS

    @pl.when(within(tile, STEPS))
    def _():
        grad_tile(z_ref, dy_ref, wd_ref, qbuf, BLOCK, lambda rows, grad: None)
        store_tile(left, qbuf, up.gbuf, lax.rem(tile, 2))

    def emit_up(unit, block):
        up_ref[:, aligned(unit, TILE)] = block

    def emit_down(unit, block):
        down_ref[pl.ds(pl.multiple_of(lax.rem(unit, 2) * HALF_ROWS, 8), HALF_ROWS), aligned(unit // 2, LANES)] = block

    tick = tile - 1

    advance(up, tile, STEPS, emit_up)
    advance(down, tick, DOWN_UNITS, emit_down)

    @pl.when(tile == 0)
    def _():
        for copy in loads(0):
            copy.start()

    @pl.when(within(tick, DOWN_UNITS - 1))
    def _():
        for copy in loads(tick + 1):
            copy.start()

    @pl.when(within(tile, STEPS))
    def _():
        up.copy(0, tile).start()

    @pl.when(within(tick, DOWN_UNITS))
    def _():
        for copy in loads(tick):
            copy.wait()
        down.copy(0, tick).start()


def ring_scratch(rows, columns):
    block = (rows, columns)
    return [
        pltpu.VMEM((2, 8, 2) + block, F32),
        pltpu.VMEM((2, 8) + block, F32),
        pltpu.VMEM((SUM_SLOTS, 8) + block, F32),
        pltpu.VMEM((SLOTS, 4) + block, F32),
        pltpu.VMEM((SLOTS, 2) + block, F32),
        pltpu.VMEM((SLOTS, 1) + block, F32),
        pltpu.SemaphoreType.DMA((4, SLOTS)),
        pltpu.SemaphoreType.DMA((4, SLOTS)),
    ]


WHOLE = pl.Buffered(buffer_count=1)
ANY = pl.BlockSpec(memory_space=pl.ANY)


def params(collective_id):
    return pltpu.CompilerParams(collective_id=collective_id, has_side_effects=True, vmem_limit_bytes=67043328, dimension_semantics=("arbitrary",))


def second_block(pre_act, grad, w_down, left, grad_down, w_up):
    last = STEPS - 1
    return pl.pallas_call(
        second_block_kernel,
        grid=(STEPS + DRAIN,),
        in_specs=[
            pl.BlockSpec((TOKENS, TILE), lambda s: (0, jnp.minimum(s, last))),
            pl.BlockSpec((TOKENS, D), lambda s: (0, 0), pipeline_mode=WHOLE),
            pl.BlockSpec((None, TILE, D), lambda s: (1, jnp.minimum(s, last), 0)),
            pl.BlockSpec((D, TOKENS), lambda s: (0, 0), pipeline_mode=WHOLE),
            ANY,
            pl.BlockSpec((None, D, TILE), lambda s: (1, 0, jnp.minimum(s, last))),
        ],
        out_specs=[pl.BlockSpec((UP_ROWS, FF), lambda s: (0, 0)), pl.BlockSpec((DOWN_ROWS, D), lambda s: (0, 0)), ANY, ANY],
        out_shape=[jax.ShapeDtypeStruct((UP_ROWS, FF), F32), jax.ShapeDtypeStruct((DOWN_ROWS, D), F32), jax.ShapeDtypeStruct((TOKENS, D), BF16), jax.ShapeDtypeStruct((D, TOKENS), BF16)],
        scratch_shapes=[pltpu.VMEM((TOKENS, TILE), BF16), pltpu.VMEM((TOKENS, D), F32), pltpu.VMEM((BLOCK, D), BF16), pltpu.VMEM((D, BLOCK), BF16)] + ring_scratch(UP_ROWS, TILE) + ring_scratch(DOWN_UNIT, D) + [pltpu.SemaphoreType.DMA((2,)), pltpu.SemaphoreType.DMA((2,))],
        compiler_params=params(1),
        cost_estimate=pl.CostEstimate(flops=6 * TOKENS * D * FF, bytes_accessed=150 * 2**20, transcendentals=2 * TOKENS * FF),
    )(pre_act, grad, w_down, left, grad_down.reshape(8, 2, DOWN_ROWS, D), w_up)


LANES = 128
HALF_ROWS = DOWN_ROWS // 2
DOWN_UNITS = 2 * D // LANES
ACT_SLOTS = 2


def first_block(pre_act, grad, w_down, grad_t, act, act_in):
    start, last = STEPS, STEPS - 1
    return pl.pallas_call(
        first_block_kernel,
        grid=(start + STEPS + DRAIN,),
        in_specs=[
            pl.BlockSpec((TOKENS, TILE), lambda s: (0, jnp.clip(s - start, 0, last))),
            pl.BlockSpec((TOKENS, D), lambda s: (0, 0), pipeline_mode=WHOLE),
            pl.BlockSpec((None, TILE, D), lambda s: (0, jnp.clip(s - start, 0, last), 0)),
            pl.BlockSpec((D, TOKENS), lambda s: (0, 0), pipeline_mode=WHOLE),
            ANY,
            pl.BlockSpec((TILE, D), lambda s: (jnp.minimum(s, TOKENS // TILE - 1), 0)),
        ],
        out_specs=[pl.BlockSpec((UP_ROWS, FF), lambda s: (0, 0)), pl.BlockSpec((DOWN_ROWS, D), lambda s: (0, 0)), ANY],
        out_shape=[jax.ShapeDtypeStruct((UP_ROWS, FF), F32), jax.ShapeDtypeStruct((DOWN_ROWS, D), F32), jax.ShapeDtypeStruct((FF, D), F32)],
        scratch_shapes=[pltpu.VMEM((TOKENS, TILE), BF16), pltpu.VMEM((D, TOKENS), BF16), pltpu.VMEM((2, TILE, D), F32), pltpu.VMEM((ACT_SLOTS, TOKENS, TILE), BF16), pltpu.SemaphoreType.DMA((ACT_SLOTS,))] + ring_scratch(UP_ROWS, TILE) + ring_scratch(HALF_ROWS, LANES) + [pltpu.SemaphoreType.DMA((2, GROUP)), pltpu.SemaphoreType.DMA((2,))],
        compiler_params=params(2),
        cost_estimate=pl.CostEstimate(flops=6 * TOKENS * D * FF, bytes_accessed=250 * 2**20, transcendentals=2 * TOKENS * FF),
    )(pre_act, grad, w_down, grad_t, act, act_in)


COLUMN_PARTS = ((0, 1664), (1664, 1664), (3328, 1536))
ROW_PARTS = ((0, 112), (112, 96), (208, 96))
ORDERS = ((2, 1, 0), (1, 0, 2), (0, 2, 1))
CHUNKS = 12


def tail_kernel(scalars, g1, g2, g3, g4, *refs):
    states, (w_up_out, w_down_out), state_outs, norm_out = refs[:6], refs[6:8], refs[8:14], refs[14]
    send_up, send_down, dir_up, dir_down, mine, stats, stat_send, stat_recv, send_sem, recv_sem, own_sem = refs[15:26]
    held, (in_sem, out_sem) = refs[26:32], refs[32:34]
    master_up, master_down, avg_up, avg_down, sq_up, sq_down = held
    fetches = [pltpu.make_async_copy(src, dst, in_sem.at[i]) for i, (src, dst) in enumerate(zip(states, held))]
    stores = [pltpu.make_async_copy(src, dst, out_sem.at[i]) for i, (src, dst) in enumerate(zip(held, state_outs))]
    for copy in fetches:
        copy.start()
    me = lax.axis_index("data")
    core = lax.rem(me, 2)
    coords = (me // 8, lax.rem(me // 4, 2), lax.rem(me // 2, 2))
    sibling = me + 1 - 2 * core
    others = [lax.rem(me + k, GROUP) for k in range(1, GROUP)]
    greet(others)

    def share(turn, row):
        mine[turn] = row
        copies = []
        for k, device in enumerate(others):
            copies.append(pltpu.make_async_remote_copy(src_ref=mine.at[turn], dst_ref=stats.at[turn, me], send_sem=stat_send.at[turn, k], recv_sem=stat_recv.at[turn, me], device_id=(device,), device_id_type=MESH))
            copies[-1].start()
        stats[turn, me] = row
        for k, device in enumerate(others):
            copies[k].wait_send()
            pltpu.make_async_remote_copy(src_ref=mine.at[turn], dst_ref=stats.at[turn, device], send_sem=stat_send.at[turn, k], recv_sem=stat_recv.at[turn, device], device_id=(device,), device_id_type=MESH).wait_recv()
        return jnp.sum(stats[turn], axis=0)

    def sum_square(values):
        return jnp.sum(values * values)

    grads = ((g1, g3), (g2, g4))
    scale = 1.0 / GROUP
    local = sum_square(g1[...] * scale) + sum_square(g3[...] * scale) + sum_square(g2[...] * scale) + sum_square(g4[...] * scale)
    total = share(0, jnp.full((8, 128), local, F32))
    norm = jnp.sqrt(total)
    clip = jnp.minimum(1.0, scalars[1] / (norm + NORM_EPS))
    norm_out[...] = norm
    clip = clip[0:1, 0:1]
    bias_one = 1.0 - BETA_ONE ** STEP
    bias_two = 1.0 - BETA_TWO ** STEP
    lane = lax.broadcasted_iota(jnp.int32, (8, 128), 1)
    row = jnp.zeros((8, 128), F32)
    families = ((master_up, avg_up, sq_up, dir_up), (master_down, avg_down, sq_down, dir_down))
    for f, (master, avg, sq, direction) in enumerate(families):
        for i in (f, 2 + f, 4 + f):
            fetches[i].wait()
        for k in range(2):
            g = grads[f][k][...] * scale
            avg_new = BETA_ONE * avg[k] + (1.0 - BETA_ONE) * clip * g
            sq_new = BETA_TWO * sq[k] + (1.0 - BETA_TWO) * (clip * clip) * (g * g)
            u = (avg_new / bias_one) / (jnp.sqrt(sq_new / bias_two) + ADAM_EPS)
            avg[k] = avg_new
            sq[k] = sq_new
            direction[k] = u
            row = row + jnp.where(lane == 2 * f + k, sum_square(master[k]), 0.0) + jnp.where(lane == 4 + 2 * f + k, sum_square(u), 0.0)
        stores[2 + f].start()
        stores[4 + f].start()
    totals = share(1, row)

    def out_view(chunk, picks, flipped=None):
        index = []
        for axis in range(3):
            if axis in picks:
                index.append(slice(None))
            elif axis == flipped:
                index.append(1 - coords[axis])
            else:
                index.append(coords[axis])
        family, k, (start, size) = chunk
        if family == 0:
            return w_up_out.at[(k, *index, core, slice(None), pl.ds(start, size))]
        return w_down_out.at[(k, *index, core, pl.ds(start, size), slice(None))]

    def neighbour(axis):
        stride = (8, 4, 2)[axis]
        return me + stride * (1 - 2 * coords[axis])

    def remote(n, kind, src, dst, device):
        return pltpu.make_async_remote_copy(src_ref=src, dst_ref=dst, send_sem=send_sem.at[n, kind], recv_sem=recv_sem.at[n, kind], device_id=(device,), device_id_type=MESH)

    chunks = []
    for f, parts in enumerate((COLUMN_PARTS, ROW_PARTS)):
        for k in range(2):
            chunks += [(f, k, part) for part in parts]
    order = [ORDERS[n % 3] for n in range(CHUNKS)]
    pending = []
    rounds = [[], [], []]
    locals_ = []
    for f, (master, direction, send) in enumerate(((master_up, dir_up, send_up), (master_down, dir_down, send_down))):
        for k in range(2):
            i = 2 * f + k
            ratio = jnp.sqrt(totals[0:1, i:i + 1]) / jnp.sqrt(totals[0:1, 4 + i:5 + i])
            new = master[k] - scalars[0] * ratio * direction[k]
            master[k] = new
            send[k] = new.astype(BF16)
            for part in range(3):
                n = 3 * i + part
                start, size = chunks[n][2]
                if f == 0:
                    src = send.at[k, :, pl.ds(start, size)]
                else:
                    src = send.at[k, pl.ds(start, size), :]
                dst = out_view(chunks[n], ())
                rounds[0].append(remote(n, 0, src, dst, neighbour(order[n][0])))
                rounds[0][-1].start()
                pending.append(remote(n, 3, src, dst, sibling))
                pending[-1].start()
                locals_.append(pltpu.make_async_copy(src, dst, own_sem.at[n]))
                locals_[-1].start()
        stores[f].start()
    for turn in range(3):
        for n in range(CHUNKS):
            first, second, third = order[n]
            if turn == 0:
                locals_[n].wait()
            rounds[turn][n].wait()
            gathered = order[n][:turn]
            view = out_view(chunks[n], gathered, order[n][turn])
            pending.append(remote(n, 4 + turn, view, view, sibling))
            pending[-1].start()
            if turn < 2:
                view = out_view(chunks[n], order[n][:turn + 1])
                rounds[turn + 1].append(remote(n, turn + 1, view, view, neighbour(order[n][turn + 1])))
                rounds[turn + 1][-1].start()
    for copy in pending + stores:
        copy.wait()


def tail(scalars, grads, states):
    vmem = pl.BlockSpec(memory_space=pltpu.VMEM)
    any_space = pl.BlockSpec(memory_space=pl.ANY)
    up, down = (2, UP_ROWS, FF), (2, DOWN_ROWS, D)
    shape = jax.ShapeDtypeStruct
    return pl.pallas_call(
        tail_kernel,
        in_specs=[pl.BlockSpec(memory_space=pltpu.SMEM)] + [vmem] * 4 + [any_space] * 6,
        out_specs=[any_space] * 8 + [vmem],
        out_shape=[
            shape((2, 2, 2, 2, 2, UP_ROWS, FF), BF16),
            shape((2, 2, 2, 2, 2, DOWN_ROWS, D), BF16),
            shape(up, F32), shape(down, F32), shape(up, F32), shape(down, F32), shape(up, F32), shape(down, F32),
            shape((8, 128), F32),
        ],
        scratch_shapes=[
            pltpu.VMEM(up, BF16), pltpu.VMEM(down, BF16), pltpu.VMEM(up, F32), pltpu.VMEM(down, F32),
            pltpu.VMEM((2, 8, 128), F32), pltpu.VMEM((2, GROUP, 8, 128), F32),
            pltpu.SemaphoreType.DMA((2, GROUP)), pltpu.SemaphoreType.DMA((2, GROUP)),
            pltpu.SemaphoreType.DMA((CHUNKS, 7)), pltpu.SemaphoreType.DMA((CHUNKS, 7)), pltpu.SemaphoreType.DMA((CHUNKS,)),
            *[pltpu.VMEM(dims, F32) for dims in (up, down) * 3], pltpu.SemaphoreType.DMA((6,)), pltpu.SemaphoreType.DMA((6,)),
        ],
        compiler_params=pltpu.CompilerParams(collective_id=3, has_side_effects=True, vmem_limit_bytes=67043328),
    )(scalars, *grads, *states)


def solution(mesh):
    batch_rows = P("data", None)
    state_rows = P(None, "data", None)
    replicated = P()

    def device_step(act_in, grad_out, w_up, w_down, master_up, master_down, exp_avg_up, exp_avg_down, exp_sq_up, exp_sq_down, learn_rate, clip_norm):
        z_one = jnp.dot(act_in, w_up[0], preferred_element_type=F32)
        act_one = gelu_parts(z_one)[0].astype(BF16)
        hidden = jnp.dot(act_one, w_down[0], preferred_element_type=F32).astype(BF16)
        z_three = jnp.dot(hidden, w_up[1], preferred_element_type=F32)
        act_three = gelu_parts(z_three)[0].astype(BF16)
        g_four = jnp.dot(act_three.T, grad_out, preferred_element_type=F32)
        shard_three, shard_four, d_hidden, d_hidden_t = second_block(z_three, grad_out, w_down, hidden.T, g_four, w_up)
        shard_one, shard_two = first_block(z_one, d_hidden, w_down, d_hidden_t, act_one, act_in)[:2]
        scalars = jnp.stack([learn_rate, clip_norm])
        outs = tail(scalars, (shard_one, shard_two, shard_three, shard_four), (master_up, master_down, exp_avg_up, exp_avg_down, exp_sq_up, exp_sq_down))
        new_w_up = outs[0].reshape(2, D, FF)
        new_w_down = outs[1].reshape(2, FF, D)
        return (new_w_up, new_w_down, *outs[2:8], outs[8][0, 0])

    return jax.shard_map(device_step, mesh=mesh, in_specs=(batch_rows, batch_rows, replicated, replicated, state_rows, state_rows, state_rows, state_rows, state_rows, state_rows, replicated, replicated), out_specs=(replicated, replicated, state_rows, state_rows, state_rows, state_rows, state_rows, state_rows, replicated), check_vma=False)
```
